256 devices in a mesh: groups: 2 (over z), seq: 64 (over x, y), mp: 2 (over core).
Axes of the slice: x: 8, y: 8, z: 2, core: 2. Of those that a mesh axis runs over, the one named last changes fastest.
The devices are a block of a 8x8x16 slice.
Arguments:
- latent_cache: bfloat16 [16384, 64, 512], P(('groups', 'seq')), parts along dimension 0, may hold values from -6 to 6
- rope_cache: bfloat16 [16384, 4096], P(('groups', 'seq')), parts along dimension 0, may hold values from -6 to 6
- q_nope: bfloat16 [16, 128, 128], P('groups', 'mp'), parts along dimension 0, may hold values from -12 to 12
- q_rope: bfloat16 [16, 128, 64], P('groups', 'mp'), parts along dimension 0, may hold values from -2000 to 2000
- w_uk: bfloat16 [128, 128, 512], P('mp', None, 'seq'), may hold values from -0.5 to 0.5
- value_up_weight: bfloat16 [128, 512, 128], P('mp', 'seq'), may hold values from -0.25 to 0.25
- w_out: bfloat16 [16384, 7168], P('mp', 'seq'), may hold values from -0.046875 to 0.046875
- page_table: int32 [16, 2048], P('groups'), parts along dimension 0, may hold values from 0 to 8191, as said below
- lengths: int32 [16], P('groups'), parts along dimension 0, may hold values from 16384 to 131072, as said below
Outputs:
- output: bfloat16 [16, 7168], P('groups', ('seq', 'mp')), parts along dimension 0
The draws below stay inside these ranges and needn't reach their ends.
There are 2 independent parts, one for each index of `groups`. The reference program is written for one: setup_inputs(seed, part) draws one part's arguments, and reference() takes and returns one part's arrays. A program takes and returns all parts, laid end to end along the dimension named above; an argument that names none is the same for every part. Nothing has to cross between parts.
Inputs may be any that keep to these rules, and one draw needn't show every extreme that they name: `lengths`: every sequence has one eighth of 131072 tokens or more; the longest has exactly 131072. page_table[b,p] for p < ceil(lengths[b] / 64) is the global slot (shard index times 128 plus local slot) holding that page; these live entries are all distinct; the other entries are 0 and unused.
All inputs are finite; a program needn't handle non-finite values.
Results may differ from the reference program's by a relative error of at most 0.012.
Values may be sent and summed in bfloat16 or wider, within the bound.
No kernel may reach another device: no remote copies, remote signals or barrier semaphores. Data moves between devices by JAX's collectives and lax.ppermute only.
A program may use at most 64 MiB of HBM per device.

```python
import jax
import jax.numpy as jnp
from jax import lax

B = 8
H = 128
NOPE = 128
ROPE = 64
KVR = 512
VDIM = 128
D = 7168
PAGE = 64
SLOTS_DEV = 128
SLOTS = 8192
MAXLEN = 131072
MAXPAGES = 2048
N_SEQ = 64


def page_layout(key):
    key_len, key_long, key_weight, key_perm = jax.random.split(jax.random.fold_in(key, 11), 4)
    others = jax.random.randint(key_len, (B,), MAXLEN // 8, MAXLEN // 4 + 1)
    longest_length = jax.random.randint(key_long, (), 0, B)
    lengths = jnp.where(jnp.arange(B) == longest_length, MAXLEN, others).astype(jnp.int32)
    page_count = (lengths + PAGE - 1) // PAGE
    offsets = jnp.cumsum(page_count) - page_count
    weight = jax.random.randint(key_weight, (N_SEQ,), 0, 4)
    shuffled = jax.random.permutation(key_perm, SLOTS)
    ranking = jnp.repeat(weight, SLOTS_DEV) * SLOTS + shuffled
    slot_order = jnp.argsort(-ranking)
    logical = jnp.arange(MAXPAGES)
    position = jnp.clip(offsets[:, None] + logical[None, :], 0, SLOTS - 1)
    page_map = jnp.where(logical[None, :] < page_count[:, None], slot_order[position], 0).astype(jnp.int32)
    return (lengths, page_map)


def rope_values(key):
    base = jnp.clip(jax.random.normal(jax.random.fold_in(key, 23), (SLOTS, PAGE, ROPE), jnp.float32), -6.0, 6.0)
    return base


def draw_lengths(key, part):
    return page_layout(key)[0]


def draw_page_table(key, part):
    return page_layout(key)[1]


def draw_rope_cache(key, part):
    return rope_values(key).reshape(SLOTS, PAGE * ROPE).astype(jnp.bfloat16)


def draw_q_rope(key, part):
    drawn = jnp.clip(2.0 * jax.random.normal(jax.random.fold_in(key, 31), (B, H, ROPE), jnp.float32), -12.0, 12.0)
    return drawn.astype(jnp.bfloat16)


def steps_of(key, dims, shards, low, high):
    gain, own = 1.0, jax.random.fold_in(key, 6)
    for dim, blocks in shards:
        steps = jnp.exp(jax.random.uniform(jax.random.fold_in(own, dim), (blocks,), jnp.float32, low / len(shards), high / len(shards)))
        gain = gain * jnp.repeat(steps, dims[dim] // blocks).reshape([-1 if axis == dim else 1 for axis in range(len(dims))])
    return gain


def gaussian(rng, extent, deviation, limit, cuts=(), held_as=jnp.bfloat16):
    gain = steps_of(rng, extent, cuts, -0.22, 0.18) if cuts else 1.0
    values = jax.random.normal(rng, extent, jnp.float32) * deviation * gain
    return jnp.minimum(jnp.maximum(values, -limit), limit).astype(held_as)


def setup_inputs(seed: int = 0, part: int = 0) -> dict:
    splits = jax.random.split(jax.random.key(seed), 10)
    part_keys = jax.random.split(jax.random.fold_in(splits[9], part), 10)
    latent_cache = gaussian(part_keys[0], (SLOTS, PAGE, KVR), 1.0, 6.0, ((0, 64),))
    rope_cache = draw_rope_cache(jax.random.fold_in(jax.random.fold_in(splits[9], part), 71), part)
    q_nope = gaussian(part_keys[2], (B, H, NOPE), 2.0, 12.0, ((1, 2),))
    q_rope = draw_q_rope(jax.random.fold_in(jax.random.fold_in(splits[9], part), 71), part)
    w_uk = gaussian(splits[4], (H, NOPE, KVR), NOPE ** -0.5, 0.5, ((0, 2), (2, 64)))
    value_up_weight = gaussian(splits[5], (H, KVR, VDIM), KVR ** -0.5, 0.25, ((0, 2), (1, 64)))
    w_out = gaussian(splits[6], (H * VDIM, D), (H * VDIM) ** -0.5, 0.046875, ((0, 2), (1, 64)))
    page_table = draw_page_table(jax.random.fold_in(jax.random.fold_in(splits[9], part), 71), part)
    lengths = draw_lengths(jax.random.fold_in(jax.random.fold_in(splits[9], part), 71), part)
    return dict(latent_cache=latent_cache, rope_cache=rope_cache, q_nope=q_nope, q_rope=q_rope, w_uk=w_uk, value_up_weight=value_up_weight, w_out=w_out, page_table=page_table, lengths=lengths)


NEG = -1.0e30


def reference(latent_cache, rope_cache, q_nope, q_rope, w_uk, value_up_weight, w_out, page_table, lengths):
    score_scale = (NOPE + ROPE) ** -0.5
    peak_score = lax.Precision.HIGHEST
    q_latent = jnp.einsum('bhn,hnk->bhk', q_nope.astype(jnp.float32), w_uk.astype(jnp.float32), precision=peak_score).astype(jnp.bfloat16)
    page_count = (lengths + PAGE - 1) // PAGE
    logical = jnp.arange(MAXPAGES, dtype=jnp.int32)
    live_page = logical[None, :] < page_count[:, None]
    tokens_in = jnp.clip(lengths[:, None] - PAGE * logical[None, :], 0, PAGE).astype(jnp.int32)
    target = jnp.where(live_page, page_table, SLOTS).astype(jnp.int32).reshape(-1)
    seq_ids = jnp.broadcast_to(jnp.arange(B, dtype=jnp.int32)[:, None], (B, MAXPAGES)).reshape(-1)
    slot_owner = jnp.zeros((SLOTS, B), jnp.float32).at[target, seq_ids].set(1.0, mode='drop')
    slot_fill = jnp.zeros((SLOTS,), jnp.int32).at[target].add(tokens_in.reshape(-1), mode='drop')
    blocks = SLOTS // 8
    latent_blocks = latent_cache.reshape(blocks, 8, PAGE, KVR)
    rope_blocks = rope_cache.reshape(blocks, 8, PAGE, ROPE)
    owner_blocks = slot_owner.reshape(blocks, 8, B)
    fill_blocks = slot_fill.reshape(blocks, 8)
    q_latent_f = q_latent.astype(jnp.float32)
    q_rope_f = q_rope.astype(jnp.float32)

    def step_block(run_state, block_data):
        run_max, run_sum, run_out = run_state
        latent_block, rope_block, owner_block, fill_block = block_data
        latent_f = latent_block.astype(jnp.float32)
        pick_latent = jnp.einsum('sb,bhk->shk', owner_block, q_latent_f, precision=peak_score)
        pick_rope = jnp.einsum('sb,bhr->shr', owner_block, q_rope_f, precision=peak_score)
        scores = (jnp.einsum('shk,stk->sht', pick_latent, latent_f, precision=peak_score)
                  + jnp.einsum('shr,str->sht', pick_rope, rope_block.astype(jnp.float32), precision=peak_score)) * score_scale
        live_token = jnp.arange(PAGE, dtype=jnp.int32)[None, None, :] < fill_block[:, None, None]
        slot_max = jnp.max(jnp.where(live_token, scores, NEG), axis=2)
        exponent = jnp.where(live_token, jnp.exp(scores - slot_max[:, :, None]), 0.0)
        slot_sum = jnp.sum(exponent, axis=2)
        weights = lax.optimization_barrier(exponent.astype(jnp.bfloat16)).astype(jnp.float32)
        slot_out = jnp.einsum('sht,stk->shk', weights, latent_f, precision=peak_score)
        owned = jnp.transpose(owner_block) > 0
        candidate = jnp.where(owned[:, :, None], slot_max[None, :, :], NEG)
        new_max = jnp.maximum(run_max, jnp.max(candidate, axis=1))
        carry_scale = jnp.exp(run_max - new_max)
        factor = jnp.where(owned[:, :, None], jnp.exp(candidate - new_max[:, None, :]), 0.0)
        run_sum = run_sum * carry_scale + jnp.einsum('bsh,sh->bh', factor, slot_sum, precision=peak_score)
        run_out = run_out * carry_scale[:, :, None] + jnp.einsum('bsh,shk->bhk', factor, slot_out, precision=peak_score)
        return (new_max, run_sum, run_out), None

    initial = (jnp.full((B, H), NEG, jnp.float32), jnp.zeros((B, H), jnp.float32), jnp.zeros((B, H, KVR), jnp.float32))
    final_state, unused = lax.scan(step_block, initial, (latent_blocks, rope_blocks, owner_blocks, fill_blocks))
    seq_max, seq_sum, seq_out = final_state
    attention_probs = (seq_out / seq_sum[:, :, None]).astype(jnp.bfloat16)
    value_rows = jnp.einsum('gre,req->grq', attention_probs.astype(jnp.float32), value_up_weight.astype(jnp.float32), precision=peak_score).astype(jnp.bfloat16)
    output = jnp.dot(value_rows.reshape(B, H * VDIM), w_out, preferred_element_type=jnp.float32).astype(jnp.bfloat16)
    return output
```

```python
import functools

import jax
import jax.numpy as jnp
from jax import lax
from jax.experimental import pallas as pl
from jax.experimental.pallas import tpu as pltpu
from jax.sharding import PartitionSpec as P

NEG = -1e30
LANES = 128
NT = (((1,), (1,)), ((), ()))


def whole(shape):
    return pl.BlockSpec(shape, lambda *_: (0,) * len(shape))


def send_query(q_ref, w_ref, v_ref, out_ref):
    seqs, heads, nope = q_ref.shape
    cols = w_ref.shape[1]
    q = q_ref[...].reshape(seqs * heads, nope)
    w = w_ref[...].reshape(heads * cols, nope)
    every = lax.dot_general(w, q, NT, preferred_element_type=jnp.float32)
    every = every.reshape(heads, cols, seqs * heads)
    head = lax.broadcasted_iota(jnp.int32, every.shape, 0)
    lane = lax.broadcasted_iota(jnp.int32, every.shape, 2)
    part = jnp.sum(jnp.where(lane % heads == head, every, 0.0), axis=0).astype(jnp.bfloat16)
    shards = out_ref.shape[0]
    tiles = seqs * heads // LANES
    for tile in range(tiles):
        piece = part[:, tile * LANES : (tile + 1) * LANES]
        out_ref[:, tile * cols : (tile + 1) * cols, :] = jnp.broadcast_to(piece[None], (shards, cols, LANES))
    out_ref[:, tiles * cols :, :] = v_ref[...]


def find_owner(page_len, first_ref, table_ref, lengths_ref, out_ref, owner_sum, fill_sum):
    seqs, pages = table_ref.shape
    slots = out_ref.shape[1]
    logical = lax.broadcasted_iota(jnp.int32, (seqs, pages), 1)
    seq = lax.broadcasted_iota(jnp.int32, (seqs, pages), 0)
    left = lengths_ref[...] - page_len * logical
    local_slot = jnp.where(left > 0, table_ref[...] - first_ref[0], -1)
    tokens = jnp.clip(left, 0, page_len)
    code = (seq * LANES + tokens).astype(jnp.float32)

    def at_slot(slot, carry):
        hit = jnp.where(local_slot == slot, code, 0.0)
        acc = hit[:, :LANES]
        for j in range(1, pages // LANES):
            acc = acc + hit[:, j * LANES : (j + 1) * LANES]
        row = jnp.sum(acc, axis=0, keepdims=True)
        owner = jnp.floor(row * (1.0 / LANES))
        owner_sum[pl.ds(slot, 1), :] = owner
        fill_sum[pl.ds(slot, 1), :] = row - owner * LANES
        return carry

    lax.fori_loop(0, slots, at_slot, 0, unroll=4)
    ones = jnp.ones((8, LANES), jnp.bfloat16)
    owner = lax.dot_general(ones, owner_sum[...].astype(jnp.bfloat16), NT, preferred_element_type=jnp.float32)
    fill = lax.dot_general(ones, fill_sum[...].astype(jnp.bfloat16), NT, preferred_element_type=jnp.float32)
    out_ref[...] = (owner * LANES + fill).astype(jnp.int32)[:1]


def attend(
    scale, chunk, code_ref, recv_ref, q_rope_ref, rope_ref, latent_hbm, out_ref,
    latent, query, scores, top, total, acc, rows, sems,
):
    slots, page_len, width = latent.shape
    seqs, heads, _ = q_rope_ref.shape
    pairs = slots // 2
    chunks = slots // chunk

    def copy_of(index):
        at = pl.ds(index * chunk, chunk)
        return pltpu.make_async_copy(latent_hbm.at[at], latent.at[at], sems.at[index])

    for index in range(chunks):
        copy_of(index).start()

    cols = recv_ref.shape[1] // (seqs * heads // LANES + 1)
    for tile in range(seqs * heads // LANES):
        block = recv_ref[:, tile * cols : (tile + 1) * cols, :].astype(jnp.float32)
        block = block.reshape(width, LANES)
        query[tile * LANES : (tile + 1) * LANES, :] = block.T.astype(jnp.bfloat16)
    top[...] = jnp.full(top.shape, NEG, jnp.float32)
    total[...] = jnp.zeros(total.shape, jnp.float32)
    acc[...] = jnp.zeros(acc.shape, jnp.float32)

    lane = lax.broadcasted_iota(jnp.int32, (heads, LANES), 1)
    left = lane < page_len

    def owners(pair):
        first, second = code_ref[0, 2 * pair], code_ref[0, 2 * pair + 1]
        return first // LANES, first % LANES, second // LANES, second % LANES

    def latent_pair(pair):
        return latent[pl.ds(2 * pair, 2)].reshape(2 * page_len, width)

    def score_pair(pair):
        a, fill_a, b, fill_b = owners(pair)
        lhs = jnp.concatenate(
            [query[pl.ds(pl.multiple_of(a * heads, heads), heads), :], query[pl.ds(pl.multiple_of(b * heads, heads), heads), :]],
            axis=0,
        )
        rot = jnp.concatenate([q_rope_ref[a], q_rope_ref[b]], axis=0)
        keys = rope_ref[pl.ds(2 * pair, 2)].reshape(2 * page_len, rope_ref.shape[2])
        both = lax.dot_general(lhs, latent_pair(pair), NT, preferred_element_type=jnp.float32)
        both = both + lax.dot_general(rot, keys, NT, preferred_element_type=jnp.float32)
        score = jnp.where(left, both[:heads], both[heads:]) * scale
        token = jnp.where(left, lane, lane - page_len)
        score = jnp.where(token < jnp.where(left, fill_a, fill_b), score, NEG)
        scores[pair] = score
        top[a] = jnp.maximum(top[a], jnp.where(left, score, NEG))
        top[b] = jnp.maximum(top[b], jnp.where(left, NEG, score))

    def score_chunk(index, carry):
        copy_of(index).wait()
        for k in range(chunk // 2):
            score_pair(index * (chunk // 2) + k)
        return carry

    lax.fori_loop(0, chunks, score_chunk, 0)

    for b in range(seqs):
        top[b] = jnp.broadcast_to(jnp.max(top[b], axis=1, keepdims=True), (heads, LANES))

    def weigh_pair(pair):
        a, _, b, _ = owners(pair)
        score = scores[pair]
        peak = jnp.where(left, top[a], top[b])
        weight = jnp.where(score > 0.5 * NEG, jnp.exp(score - peak), 0.0)
        weight_a = jnp.where(left, weight, 0.0)
        weight_b = jnp.where(left, 0.0, weight)
        total[a] = total[a] + weight_a
        total[b] = total[b] + weight_b
        lhs = jnp.concatenate([weight_a, weight_b], axis=0).astype(jnp.bfloat16)
        both = jnp.dot(lhs, latent_pair(pair), preferred_element_type=jnp.float32)
        acc[a] = acc[a] + both[:heads]
        acc[b] = acc[b] + both[heads:]

    def weigh_chunk(index, carry):
        for k in range(chunk // 2):
            weigh_pair(index * (chunk // 2) + k)
        return carry

    lax.fori_loop(0, chunks, weigh_chunk, 0)

    for piece in range(width // LANES + 1):
        for b in range(seqs):
            if piece < width // LANES:
                value = acc[b, :, piece * LANES : (piece + 1) * LANES]
            else:
                sums = jnp.broadcast_to(jnp.sum(total[b], axis=1, keepdims=True), (heads, LANES))
                value = jnp.where(lane < 3, top[b], sums)
            rows[pl.ds(b, heads, stride=seqs), :] = value
        value = rows[...]
        if piece == width // LANES:
            high = value.astype(jnp.bfloat16).astype(jnp.float32)
            middle = (value - high).astype(jnp.bfloat16).astype(jnp.float32)
            low = value - high - middle
            third = lax.broadcasted_iota(jnp.int32, value.shape, 1) % 3
            value = jnp.where(third == 0, high, jnp.where(third == 1, middle, low))
        out_ref[:, :, piece * LANES : (piece + 1) * LANES] = value.reshape(heads, seqs, LANES).astype(jnp.bfloat16)


def combine(width, peers_ref, up_ref, out_ref):
    shards, seqs, _ = peers_ref.shape
    stats = peers_ref[:, :, width:].astype(jnp.float32)
    lane = lax.broadcasted_iota(jnp.int32, stats.shape, 2)
    peak = jnp.sum(jnp.where(lane < 3, stats, 0.0), axis=2, keepdims=True)
    sums = jnp.sum(jnp.where((lane >= 3) & (lane < 6), stats, 0.0), axis=2, keepdims=True)
    rescale = jnp.exp(peak - jnp.max(peak, axis=0, keepdims=True))
    total = jnp.sum(sums * rescale, axis=0)
    mixed = jnp.sum(peers_ref[:, :, :width].astype(jnp.float32) * rescale, axis=0)
    attention = (mixed / total).astype(jnp.bfloat16)
    up = up_ref[...].astype(jnp.float32).reshape(width, up_ref.shape[2]).astype(jnp.bfloat16)
    values = jnp.dot(attention, up, preferred_element_type=jnp.float32).astype(jnp.bfloat16)
    out_ref[...] = jnp.broadcast_to(values[None], out_ref.shape)


def local(
    latent_cache, rope_cache, q_nope, q_rope, w_uk, value_up_weight, w_out, page_table, lengths
):
    slots, page_len, width = latent_cache.shape
    seqs, heads, nope = q_nope.shape
    rope = q_rope.shape[2]
    value_dim = value_up_weight.shape[2]
    cols = w_uk.shape[2]
    shards = lax.axis_size("seq")
    pages = page_table.shape[1]
    scale = (nope + rope) ** -0.5
    f32, bf16 = jnp.float32, jnp.bfloat16

    send_rows = (seqs * heads // LANES + 1) * cols
    sent = pl.pallas_call(
        send_query, out_shape=jax.ShapeDtypeStruct((shards, send_rows, LANES), bf16)
    )(q_nope, jnp.swapaxes(w_uk, 1, 2), value_up_weight)
    recv = lax.all_to_all(sent, "seq", 0, 0, tiled=True)

    first = (lax.axis_index("seq") * slots).astype(jnp.int32).reshape(1)
    code = pl.pallas_call(
        functools.partial(find_owner, page_len),
        out_shape=jax.ShapeDtypeStruct((1, slots), jnp.int32),
        in_specs=[
            pl.BlockSpec(memory_space=pltpu.SMEM),
            whole((seqs, pages)),
            whole((seqs, 1)),
        ],
        scratch_shapes=[pltpu.VMEM((slots, LANES), f32), pltpu.VMEM((slots, LANES), f32)],
    )(first, page_table, lengths.reshape(seqs, 1))
    rope_keys = rope_cache.reshape(slots, page_len, rope)

    chunk = 8
    out_width = width + LANES
    partial = pl.pallas_call(
        functools.partial(attend, scale, chunk),
        out_shape=jax.ShapeDtypeStruct((heads, seqs, out_width), bf16),
        in_specs=[
            pl.BlockSpec(memory_space=pltpu.SMEM),
            whole(recv.shape),
            whole(q_rope.shape),
            whole(rope_keys.shape),
            pl.BlockSpec(memory_space=pl.ANY),
        ],
        scratch_shapes=[
            pltpu.VMEM((slots, page_len, width), bf16),
            pltpu.VMEM((seqs * heads, width), bf16),
            pltpu.VMEM((slots // 2, heads, LANES), f32),
            pltpu.VMEM((seqs, heads, LANES), f32),
            pltpu.VMEM((seqs, heads, LANES), f32),
            pltpu.VMEM((seqs, heads, width), f32),
            pltpu.VMEM((seqs * heads, LANES), f32),
            pltpu.SemaphoreType.DMA((slots // chunk,)),
        ],
    )(code, recv, q_rope, rope_keys, latent_cache)
    peers = lax.all_to_all(partial, "seq", 0, 0, tiled=True)

    last = send_rows // cols - 1
    values = pl.pallas_call(
        functools.partial(combine, width),
        out_shape=jax.ShapeDtypeStruct((shards, seqs, value_dim), bf16),
        grid=(1,),
        in_specs=[
            whole(peers.shape),
            pl.BlockSpec((shards, cols, LANES), lambda i: (0, last, 0)),
        ],
        out_specs=whole((shards, seqs, value_dim)),
    )(peers, recv)
    every = lax.all_to_all(values, "seq", 0, 0, tiled=True)
    flat = jnp.swapaxes(every, 0, 1).reshape(seqs, heads * value_dim)
    half = jnp.dot(flat, w_out, preferred_element_type=f32)
    both = half + lax.ppermute(half, "mp", [(0, 1), (1, 0)])
    share = half.shape[1] // lax.axis_size("mp")
    return lax.dynamic_slice_in_dim(both, lax.axis_index("mp") * share, share, 1).astype(bf16)


def solution(mesh):
    return jax.shard_map(
        local,
        mesh=mesh,
        in_specs=(
            P(("groups", "seq"), None, None),
            P(("groups", "seq"), None),
            P("groups", "mp", None),
            P("groups", "mp", None),
            P("mp", None, "seq"),
            P("mp", "seq", None),
            P("mp", "seq"),
            P("groups", None),
            P("groups"),
        ),
        out_specs=P("groups", ("seq", "mp")),
        check_vma=False,
    )
```

```python
import functools

import jax
import jax.numpy as jnp
from jax import lax
from jax.experimental import pallas as pl
from jax.experimental.pallas import tpu as pltpu
from jax.sharding import PartitionSpec as P

NEG = -1e30
LANES = 128
GROUP = 4
BATCH = 4
NT = (((1,), (1,)), ((), ()))


def whole(shape):
    return pl.BlockSpec(shape, lambda *_: (0,) * len(shape))


def room(mib):
    return pltpu.CompilerParams(vmem_limit_bytes=mib * 1024 * 1024)


def send_query(q_ref, w_ref, v_ref, out_ref):
    seqs, heads, nope = q_ref.shape
    cols = w_ref.shape[1]
    q = q_ref[...].reshape(seqs * heads, nope)
    w = w_ref[...].reshape(heads * cols, nope)
    every = lax.dot_general(w, q, NT, preferred_element_type=jnp.float32)
    every = every.reshape(heads, cols, seqs * heads)
    head = lax.broadcasted_iota(jnp.int32, every.shape, 0)
    lane = lax.broadcasted_iota(jnp.int32, every.shape, 2)
    part = jnp.sum(jnp.where(lane % heads == head, every, 0.0), axis=0).astype(jnp.bfloat16)
    shards = out_ref.shape[0]
    tiles = seqs * heads // LANES
    for tile in range(tiles):
        piece = part[:, tile * LANES : (tile + 1) * LANES]
        out_ref[:, tile * cols : (tile + 1) * cols, :] = jnp.broadcast_to(piece[None], (shards, cols, LANES))
    out_ref[:, tiles * cols :, :] = v_ref[...]


def order_slots(page_len, first_ref, table_ref, lengths_ref, out_ref, owner_sum, fill_sum):
    seqs, pages = table_ref.shape
    slots = owner_sum.shape[0]
    places = out_ref.shape[1]
    f32, bf16 = jnp.float32, jnp.bfloat16
    logical = lax.broadcasted_iota(jnp.int32, (seqs, pages), 1)
    seq = lax.broadcasted_iota(jnp.int32, (seqs, pages), 0)
    left = lengths_ref[...] - page_len * logical
    local_slot = jnp.where(left > 0, table_ref[...] - first_ref[0], -1)
    tokens = jnp.clip(left, 0, page_len)
    code = (seq * LANES + tokens).astype(f32)

    def at_slot(slot, carry):
        hit = jnp.where(local_slot == slot, code, 0.0)
        acc = hit[:, :LANES]
        for j in range(1, pages // LANES):
            acc = acc + hit[:, j * LANES : (j + 1) * LANES]
        row = jnp.sum(acc, axis=0, keepdims=True)
        owner = jnp.floor(row * (1.0 / LANES))
        owner_sum[pl.ds(slot, 1), :] = owner
        fill_sum[pl.ds(slot, 1), :] = row - owner * LANES
        return carry

    lax.fori_loop(0, slots, at_slot, 0, unroll=4)
    ones = jnp.ones((8, LANES), bf16)
    owner = lax.dot_general(ones, owner_sum[...].astype(bf16), NT, preferred_element_type=f32)
    fill = lax.dot_general(ones, fill_sum[...].astype(bf16), NT, preferred_element_type=f32)

    row = lax.broadcasted_iota(jnp.int32, (seqs, slots), 0)
    slot = lax.broadcasted_iota(jnp.int32, (seqs, slots), 1)
    mine = (owner[:seqs] == row.astype(f32)) & (fill[:seqs] > 0.0)
    ours = jnp.where(mine, 1.0, 0.0)
    before = lax.broadcasted_iota(jnp.int32, (slots, slots), 0) < lax.broadcasted_iota(
        jnp.int32, (slots, slots), 1
    )
    rank = jnp.dot(ours.astype(bf16), jnp.where(before, 1.0, 0.0).astype(bf16), preferred_element_type=f32)
    count = jnp.broadcast_to(jnp.sum(ours, axis=1, keepdims=True), (seqs, slots))
    groups = jnp.floor((count + (GROUP - 1)) * (1.0 / GROUP))
    base, starts = jnp.zeros((1, slots), f32), []
    for b in range(seqs):
        starts.append(base)
        base = base + groups[b : b + 1]
    place = GROUP * jnp.concatenate(starts, axis=0) + rank
    place = jnp.sum(jnp.where(mine, place + 1.0, 0.0), axis=0, keepdims=True) - 1.0
    at = lax.broadcasted_iota(jnp.int32, (places, slots), 0).astype(f32) == place
    value = jnp.where(row == 0, slot.astype(f32), jnp.where(row == 1, fill[:seqs], owner[:seqs]))
    found = lax.dot_general(
        value.astype(bf16), jnp.where(at, 1.0, 0.0).astype(bf16), NT, preferred_element_type=f32
    )
    packed = (found[2:3] * LANES + found[0:1]) * LANES + found[1:2]
    place = lax.broadcasted_iota(jnp.int32, (1, places), 1)
    total = jnp.concatenate([base] * (places // slots), axis=1)
    out_ref[...] = jnp.where(place == places - 1, total, packed).astype(jnp.int32)


def steps_of(order_ref, batch):
    return (order_ref[0, order_ref.shape[1] - 1] + (batch - 1)) // batch


def slot_at(order_ref, group, k):
    code = order_ref[0, GROUP * group + k]
    return (code // LANES) % LANES, code % LANES


def owner_of(order_ref, group):
    return order_ref[0, GROUP * group] // (LANES * LANES)


def score_rope(scale, page_len, order_ref, q_ref, key_ref, out_ref):
    heads = q_ref.shape[1]
    lane = lax.broadcasted_iota(jnp.int32, (heads, GROUP * page_len), 1)

    def score(step, carry):
        for j in range(BATCH):
            group = step * BATCH + j
            keys, limit = [], None
            for k in range(GROUP):
                slot, fill = slot_at(order_ref, group, k)
                keys.append(key_ref[slot])
                end = k * page_len + fill
                limit = end if limit is None else jnp.where(lane >= k * page_len, end, limit)
            keys = jnp.concatenate(keys, axis=0)
            both = lax.dot_general(
                q_ref[owner_of(order_ref, group)], keys, NT, preferred_element_type=jnp.float32
            )
            out_ref[group] = jnp.where(lane < limit, both * scale, NEG)
        return carry

    lax.fori_loop(0, steps_of(order_ref, BATCH), score, 0)


def attend(
    scale, page_len, order_ref, recv_ref, rope_hbm, latent_hbm, out_ref, up_ref,
    latent, query, scores, top, total, acc, rows, sems, rope_sems,
):
    _, tokens, width = latent.shape
    seqs, heads, _ = top.shape
    steps = steps_of(order_ref, BATCH)

    def fetch(step):
        for j in range(BATCH):
            group = step * BATCH + j
            for k in range(GROUP):
                slot, _ = slot_at(order_ref, group, k)
                pltpu.make_async_copy(
                    latent_hbm.at[slot], latent.at[group, pl.ds(k * page_len, page_len)], sems.at[group]
                ).start()
            pltpu.make_async_copy(rope_hbm.at[group], scores.at[group], rope_sems.at[group]).start()

    ahead = 3
    for step in range(ahead):

        @pl.when(step < steps)
        def _():
            fetch(step)

    cols = recv_ref.shape[1] // (seqs * heads // LANES + 1)
    for tile in range(seqs * heads // LANES):
        block = recv_ref[:, tile * cols : (tile + 1) * cols, :].astype(jnp.float32)
        block = block.reshape(width, LANES)
        query[tile * LANES : (tile + 1) * LANES, :] = block.T.astype(jnp.bfloat16)
    up_ref[...] = recv_ref[:, recv_ref.shape[1] - cols :, :]
    top[...] = jnp.full(top.shape, NEG, jnp.float32)
    total[...] = jnp.zeros(total.shape, jnp.float32)
    acc[...] = jnp.zeros(acc.shape, jnp.float32)

    def score(step, carry):
        @pl.when(step + ahead < steps)
        def _():
            fetch(step + ahead)

        for j in range(BATCH):
            group = step * BATCH + j
            pltpu.make_async_copy(latent.at[group], latent.at[group], sems.at[group]).wait()
            pltpu.make_async_copy(rope_hbm.at[group], scores.at[group], rope_sems.at[group]).wait()
        made = []
        for j in range(BATCH):
            group = step * BATCH + j
            b = owner_of(order_ref, group)
            lhs = query[pl.ds(pl.multiple_of(b * heads, heads), heads), :]
            both = lax.dot_general(lhs, latent[group], NT, preferred_element_type=jnp.float32)
            made.append((group, b, both * scale + scores[group]))
        for group, b, both in made:
            scores[group] = both
            high = both[:, :LANES]
            for k in range(1, tokens // LANES):
                high = jnp.maximum(high, both[:, k * LANES : (k + 1) * LANES])
            top[b] = jnp.maximum(top[b], high)
        return carry

    lax.fori_loop(0, steps, score, 0)

    for b in range(seqs):
        top[b] = jnp.broadcast_to(jnp.max(top[b], axis=1, keepdims=True), (heads, LANES))

    def weigh(step, carry):
        made = []
        for j in range(BATCH):
            group = step * BATCH + j
            b = owner_of(order_ref, group)
            both = scores[group]
            peak = top[b]
            parts, some = [], None
            for k in range(tokens // LANES):
                part = both[:, k * LANES : (k + 1) * LANES]
                part = jnp.where(part > 0.5 * NEG, jnp.exp(part - peak), 0.0)
                some = part if some is None else some + part
                parts.append(part.astype(jnp.bfloat16))
            lhs = jnp.concatenate(parts, axis=1)
            made.append((b, some, jnp.dot(lhs, latent[group], preferred_element_type=jnp.float32)))
        for b, some, out in made:
            total[b] = total[b] + some
            acc[b] = acc[b] + out
        return carry

    lax.fori_loop(0, steps, weigh, 0)

    lane = lax.broadcasted_iota(jnp.int32, (heads, LANES), 1)
    for piece in range(width // LANES + 1):
        for b in range(seqs):
            if piece < width // LANES:
                value = acc[b, :, piece * LANES : (piece + 1) * LANES]
            else:
                sums = jnp.broadcast_to(jnp.sum(total[b], axis=1, keepdims=True), (heads, LANES))
                value = jnp.where(lane < 3, top[b], sums)
            rows[piece % 2, pl.ds(b, heads, stride=seqs), :] = value
        value = rows[piece % 2]
        if piece == width // LANES:
            high = value.astype(jnp.bfloat16).astype(jnp.float32)
            middle = (value - high).astype(jnp.bfloat16).astype(jnp.float32)
            low = value - high - middle
            third = lax.broadcasted_iota(jnp.int32, value.shape, 1) % 3
            value = jnp.where(third == 0, high, jnp.where(third == 1, middle, low))
        out_ref[:, :, piece * LANES : (piece + 1) * LANES] = value.reshape(heads, seqs, LANES).astype(jnp.bfloat16)


def combine(width, peers_ref, up_ref, out_ref):
    shards, seqs, _ = peers_ref.shape
    stats = peers_ref[:, :, width:].astype(jnp.float32)
    lane = lax.broadcasted_iota(jnp.int32, stats.shape, 2)
    peak = jnp.sum(jnp.where(lane < 3, stats, 0.0), axis=2, keepdims=True)
    sums = jnp.sum(jnp.where((lane >= 3) & (lane < 6), stats, 0.0), axis=2, keepdims=True)
    rescale = jnp.exp(peak - jnp.max(peak, axis=0, keepdims=True))
    total = jnp.sum(sums * rescale, axis=0)
    mixed = jnp.sum(peers_ref[:, :, :width].astype(jnp.float32) * rescale, axis=0)
    attention = (mixed / total).astype(jnp.bfloat16)
    up = up_ref[...].astype(jnp.float32).reshape(width, up_ref.shape[2]).astype(jnp.bfloat16)
    values = jnp.dot(attention, up, preferred_element_type=jnp.float32).astype(jnp.bfloat16)
    out_ref[...] = jnp.broadcast_to(values[None], out_ref.shape)


def local(
    latent_cache, rope_cache, q_nope, q_rope, w_uk, value_up_weight, w_out, page_table, lengths
):
    slots, page_len, width = latent_cache.shape
    seqs, heads, nope = q_nope.shape
    rope = q_rope.shape[2]
    value_dim = value_up_weight.shape[2]
    cols = w_uk.shape[2]
    shards = lax.axis_size("seq")
    pages = page_table.shape[1]
    scale = (nope + rope) ** -0.5
    f32, bf16 = jnp.float32, jnp.bfloat16

    send_rows = (seqs * heads // LANES + 1) * cols
    sent = pl.pallas_call(
        send_query,
        out_shape=jax.ShapeDtypeStruct((shards, send_rows, LANES), bf16),
        compiler_params=room(8),
    )(q_nope, jnp.swapaxes(w_uk, 1, 2), value_up_weight)
    recv = lax.all_to_all(sent, "seq", 0, 0, tiled=True)

    first = (lax.axis_index("seq") * slots).astype(jnp.int32).reshape(1)
    most = (slots + seqs * (GROUP - 1)) // GROUP
    most = (most + BATCH - 1) // BATCH * BATCH
    places = (most * GROUP) // slots * slots + slots
    smem = pl.BlockSpec(memory_space=pltpu.SMEM)
    order = pl.pallas_call(
        functools.partial(order_slots, page_len),
        out_shape=jax.ShapeDtypeStruct((1, places), jnp.int32),
        in_specs=[smem, whole((seqs, pages)), whole((seqs, 1))],
        scratch_shapes=[pltpu.VMEM((slots, LANES), f32), pltpu.VMEM((slots, LANES), f32)],
        compiler_params=room(4),
    )(first, page_table, lengths.reshape(seqs, 1))
    rope_keys = rope_cache.reshape(slots, page_len, rope)
    tokens = GROUP * page_len
    rope_score = pl.pallas_call(
        functools.partial(score_rope, scale, page_len),
        out_shape=jax.ShapeDtypeStruct((most, heads, tokens), f32),
        in_specs=[smem, whole(q_rope.shape), whole(rope_keys.shape)],
        compiler_params=room(8),
    )(order, q_rope, rope_keys)

    out_width = width + LANES
    partial, up = pl.pallas_call(
        functools.partial(attend, scale, page_len),
        out_shape=(
            jax.ShapeDtypeStruct((heads, seqs, out_width), bf16),
            jax.ShapeDtypeStruct((shards, cols, LANES), bf16),
        ),
        in_specs=[
            smem,
            whole(recv.shape),
            pl.BlockSpec(memory_space=pltpu.HBM),
            pl.BlockSpec(memory_space=pltpu.HBM),
        ],
        scratch_shapes=[
            pltpu.VMEM((most, tokens, width), bf16),
            pltpu.VMEM((seqs * heads, width), bf16),
            pltpu.VMEM((most, heads, tokens), f32),
            pltpu.VMEM((seqs, heads, LANES), f32),
            pltpu.VMEM((seqs, heads, LANES), f32),
            pltpu.VMEM((seqs, heads, width), f32),
            pltpu.VMEM((2, seqs * heads, LANES), f32),
            pltpu.SemaphoreType.DMA((most,)),
            pltpu.SemaphoreType.DMA((most,)),
        ],
        compiler_params=room(52),
    )(order, recv, rope_score, latent_cache)
    peers = lax.all_to_all(partial, "seq", 0, 0, tiled=True)

    values = pl.pallas_call(
        functools.partial(combine, width),
        out_shape=jax.ShapeDtypeStruct((shards, seqs, value_dim), bf16),
        compiler_params=room(8),
    )(peers, up)
    every = lax.all_to_all(values, "seq", 0, 0, tiled=True)
    flat = jnp.swapaxes(every, 0, 1).reshape(seqs, heads * value_dim)
    half = jnp.dot(flat, w_out, preferred_element_type=f32)
    both = half + lax.ppermute(half, "mp", [(0, 1), (1, 0)])
    share = half.shape[1] // lax.axis_size("mp")
    return lax.dynamic_slice_in_dim(both, lax.axis_index("mp") * share, share, 1).astype(bf16)


def solution(mesh):
    return jax.shard_map(
        local,
        mesh=mesh,
        in_specs=(
            P(("groups", "seq"), None, None),
            P(("groups", "seq"), None),
            P("groups", "mp", None),
            P("groups", "mp", None),
            P("mp", None, "seq"),
            P("mp", "seq", None),
            P("mp", "seq"),
            P("groups", None),
            P("groups"),
        ),
        out_specs=P("groups", ("seq", "mp")),
        check_vma=False,
    )
```

```python
import functools

import jax
import jax.numpy as jnp
from jax import lax
from jax.experimental import pallas as pl
from jax.experimental.pallas import tpu as pltpu
from jax.sharding import PartitionSpec as P

NEG = -1e30
LANES = 128
GROUP = 4
BATCH = 4
NT = (((1,), (1,)), ((), ()))


def whole(shape):
    return pl.BlockSpec(shape, lambda *_: (0,) * len(shape))


def room(mib):
    return pltpu.CompilerParams(vmem_limit_bytes=mib * 1024 * 1024)


def hbm(x):
    return pltpu.with_memory_space_constraint(x, pltpu.HBM)


def send_query(q_hbm, w_hbm, v_hbm, out_ref, q_ref, w_ref, v_ref, sems):
    seqs, heads, nope = q_ref.shape
    cols = w_ref.shape[1]
    moves = [
        pltpu.make_async_copy(source, target, sems.at[i])
        for i, (source, target) in enumerate(((q_hbm, q_ref), (w_hbm, w_ref), (v_hbm, v_ref)))
    ]
    for move in moves:
        move.start()
    for move in moves:
        move.wait()
    q = q_ref[...].reshape(seqs * heads, nope)
    w = w_ref[...].reshape(heads * cols, nope)
    every = lax.dot_general(w, q, NT, preferred_element_type=jnp.float32)
    every = every.reshape(heads, cols, seqs * heads)
    head = lax.broadcasted_iota(jnp.int32, every.shape, 0)
    lane = lax.broadcasted_iota(jnp.int32, every.shape, 2)
    part = jnp.sum(jnp.where(lane % heads == head, every, 0.0), axis=0).astype(jnp.bfloat16)
    shards = out_ref.shape[0]
    tiles = seqs * heads // LANES
    for tile in range(tiles):
        piece = part[:, tile * LANES : (tile + 1) * LANES]
        out_ref[:, tile * cols : (tile + 1) * cols, :] = jnp.broadcast_to(piece[None], (shards, cols, LANES))
    out_ref[:, tiles * cols :, :] = v_ref[...]


def order_slots(page_len, first_ref, lengths_ref, table_hbm, out_ref, table_ref, owner_sum, fill_sum, sem):
    seqs, pages = table_ref.shape
    slots = owner_sum.shape[0]
    places = out_ref.shape[1]
    f32, bf16 = jnp.float32, jnp.bfloat16
    logical = lax.broadcasted_iota(jnp.int32, (seqs, pages), 1)
    seq = lax.broadcasted_iota(jnp.int32, (seqs, pages), 0)
    move = pltpu.make_async_copy(table_hbm, table_ref, sem)
    move.start()
    length = jnp.zeros((seqs, pages), jnp.int32)
    for b in range(seqs):
        length = jnp.where(seq == b, lengths_ref[b], length)
    left = length - page_len * logical
    move.wait()
    local_slot = jnp.where(left > 0, table_ref[...] - first_ref[0], -1)
    tokens = jnp.clip(left, 0, page_len)
    code = (seq * LANES + tokens).astype(f32)

    def at_slot(slot, carry):
        hit = jnp.where(local_slot == slot, code, 0.0)
        acc = hit[:, :LANES]
        for j in range(1, pages // LANES):
            acc = acc + hit[:, j * LANES : (j + 1) * LANES]
        row = jnp.sum(acc, axis=0, keepdims=True)
        owner = jnp.floor(row * (1.0 / LANES))
        owner_sum[pl.ds(slot, 1), :] = owner
        fill_sum[pl.ds(slot, 1), :] = row - owner * LANES
        return carry

    lax.fori_loop(0, slots, at_slot, 0, unroll=4)
    ones = jnp.ones((8, LANES), bf16)
    owner = lax.dot_general(ones, owner_sum[...].astype(bf16), NT, preferred_element_type=f32)
    fill = lax.dot_general(ones, fill_sum[...].astype(bf16), NT, preferred_element_type=f32)

    row = lax.broadcasted_iota(jnp.int32, (seqs, slots), 0)
    slot = lax.broadcasted_iota(jnp.int32, (seqs, slots), 1)
    mine = (owner[:seqs] == row.astype(f32)) & (fill[:seqs] > 0.0)
    ours = jnp.where(mine, 1.0, 0.0)
    before = lax.broadcasted_iota(jnp.int32, (slots, slots), 0) < lax.broadcasted_iota(
        jnp.int32, (slots, slots), 1
    )
    rank = jnp.dot(ours.astype(bf16), jnp.where(before, 1.0, 0.0).astype(bf16), preferred_element_type=f32)
    count = jnp.broadcast_to(jnp.sum(ours, axis=1, keepdims=True), (seqs, slots))
    groups = jnp.floor((count + (GROUP - 1)) * (1.0 / GROUP))
    base, starts = jnp.zeros((1, slots), f32), []
    for b in range(seqs):
        starts.append(base)
        base = base + groups[b : b + 1]
    place = GROUP * jnp.concatenate(starts, axis=0) + rank
    place = jnp.sum(jnp.where(mine, place + 1.0, 0.0), axis=0, keepdims=True) - 1.0
    at = lax.broadcasted_iota(jnp.int32, (places, slots), 0).astype(f32) == place
    value = jnp.where(row == 0, slot.astype(f32), jnp.where(row == 1, fill[:seqs], owner[:seqs]))
    found = lax.dot_general(
        value.astype(bf16), jnp.where(at, 1.0, 0.0).astype(bf16), NT, preferred_element_type=f32
    )
    packed = (found[2:3] * LANES + found[0:1]) * LANES + found[1:2]
    place = lax.broadcasted_iota(jnp.int32, (1, places), 1)
    total = jnp.concatenate([base] * (places // slots), axis=1)
    out_ref[...] = jnp.where(place == places - 1, total, packed).astype(jnp.int32)


SHIFT = 7


def steps_of(order_ref, batch):
    return (order_ref[0, order_ref.shape[1] - 1] + (batch - 1)) // batch


def slot_at(order_ref, group, k):
    code = order_ref[0, GROUP * group + k]
    return lax.shift_right_logical(code, SHIFT) & (LANES - 1), code & (LANES - 1)


def owner_of(order_ref, group):
    return lax.shift_right_logical(order_ref[0, GROUP * group], 2 * SHIFT)


def score_rope(
    scale, page_len, order_ref, q_hbm, tiles_hbm, out_ref, q_ref, tiles, flat, spread, keys, sems
):
    heads, rope = q_ref.shape[1:]
    blocks, pairs, _, _ = tiles.shape
    first = pltpu.make_async_copy(q_hbm, q_ref, sems.at[0])
    second = pltpu.make_async_copy(tiles_hbm, tiles, sems.at[1])
    first.start()
    second.start()
    first.wait()
    second.wait()
    even = lax.broadcasted_iota(jnp.int32, (pairs, LANES), 1) < rope

    def spread_block(block, carry):
        flat[...] = tiles[block].astype(jnp.float32).reshape(pairs * 8, LANES)
        for k in range(8):
            two = flat[pl.ds(k, pairs, stride=8), :]
            spread[k, pl.ds(0, pairs, stride=2), :] = jnp.where(even, two, 0.0)
            spread[k, pl.ds(1, pairs, stride=2), :] = jnp.where(even, 0.0, two)
        keys[pl.ds(block * 8, 8)] = spread[...].astype(jnp.bfloat16)
        return carry

    lax.fori_loop(0, blocks, spread_block, 0)
    lane = lax.broadcasted_iota(jnp.int32, (heads, GROUP * page_len), 1)

    def score(step, carry):
        for j in range(BATCH):
            group = step * BATCH + j
            rows, limit = [], None
            for k in range(GROUP):
                slot, fill = slot_at(order_ref, group, k)
                rows.append(keys[slot])
                end = k * page_len + fill
                limit = end if limit is None else jnp.where(lane >= k * page_len, end, limit)
            query = q_ref[owner_of(order_ref, group)].astype(jnp.float32)
            query = jnp.concatenate([query, query], axis=1).astype(jnp.bfloat16)
            both = lax.dot_general(
                query, jnp.concatenate(rows, axis=0), NT, preferred_element_type=jnp.float32
            )
            out_ref[group] = jnp.where(lane < limit, both * scale, NEG)
        return carry

    lax.fori_loop(0, steps_of(order_ref, BATCH), score, 0)


def attend(
    scale, page_len, order_ref, recv_ref, rope_hbm, latent_hbm, out_ref, up_ref,
    latent, query, scores, top, total, acc, rows, sems, rope_sems,
):
    _, tokens, width = latent.shape
    seqs, heads, _ = top.shape
    steps = steps_of(order_ref, BATCH)

    def fetch(step):
        for j in range(BATCH):
            group = step * BATCH + j
            for k in range(GROUP):
                slot, _ = slot_at(order_ref, group, k)
                pltpu.make_async_copy(
                    latent_hbm.at[slot], latent.at[group, pl.ds(k * page_len, page_len)], sems.at[step]
                ).start()
        batch = pl.ds(step * BATCH, BATCH)
        pltpu.make_async_copy(rope_hbm.at[batch], scores.at[batch], rope_sems.at[step]).start()

    ahead = 3
    for step in range(ahead):

        @pl.when(step < steps)
        def _():
            fetch(step)

    cols = recv_ref.shape[1] // (seqs * heads // LANES + 1)
    for tile in range(seqs * heads // LANES):
        block = recv_ref[:, tile * cols : (tile + 1) * cols, :].astype(jnp.float32)
        block = block.reshape(width, LANES)
        query[tile * LANES : (tile + 1) * LANES, :] = block.T.astype(jnp.bfloat16)
    up_ref[...] = recv_ref[:, recv_ref.shape[1] - cols :, :]
    top[...] = jnp.full(top.shape, NEG, jnp.float32)
    total[...] = jnp.zeros(total.shape, jnp.float32)
    acc[...] = jnp.zeros(acc.shape, jnp.float32)

    def score(step, carry):
        @pl.when(step + ahead < steps)
        def _():
            fetch(step + ahead)

        batch = pl.ds(step * BATCH, BATCH)
        pltpu.make_async_copy(latent.at[batch], latent.at[batch], sems.at[step]).wait()
        pltpu.make_async_copy(rope_hbm.at[batch], scores.at[batch], rope_sems.at[step]).wait()
        made = []
        for j in range(BATCH):
            group = step * BATCH + j
            b = owner_of(order_ref, group)
            lhs = query[pl.ds(pl.multiple_of(b * heads, heads), heads), :]
            both = lax.dot_general(lhs, latent[group], NT, preferred_element_type=jnp.float32)
            made.append((group, b, both * scale + scores[group]))
        for group, b, both in made:
            scores[group] = both
            high = both[:, :LANES]
            for k in range(1, tokens // LANES):
                high = jnp.maximum(high, both[:, k * LANES : (k + 1) * LANES])
            top[b] = jnp.maximum(top[b], high)
        return carry

    lax.fori_loop(0, steps, score, 0)

    for b in range(seqs):
        top[b] = jnp.broadcast_to(jnp.max(top[b], axis=1, keepdims=True), (heads, LANES))

    def weigh(step, carry):
        made = []
        for j in range(BATCH):
            group = step * BATCH + j
            b = owner_of(order_ref, group)
            both = scores[group]
            peak = top[b]
            parts, some = [], None
            for k in range(tokens // LANES):
                part = both[:, k * LANES : (k + 1) * LANES]
                part = jnp.where(part > 0.5 * NEG, jnp.exp(part - peak), 0.0)
                some = part if some is None else some + part
                parts.append(part.astype(jnp.bfloat16))
            lhs = jnp.concatenate(parts, axis=1)
            made.append((b, some, jnp.dot(lhs, latent[group], preferred_element_type=jnp.float32)))
        for b, some, out in made:
            total[b] = total[b] + some
            acc[b] = acc[b] + out
        return carry

    lax.fori_loop(0, steps, weigh, 0)

    lane = lax.broadcasted_iota(jnp.int32, (heads, LANES), 1)
    for piece in range(width // LANES + 1):
        for b in range(seqs):
            if piece < width // LANES:
                value = acc[b, :, piece * LANES : (piece + 1) * LANES]
            else:
                sums = jnp.broadcast_to(jnp.sum(total[b], axis=1, keepdims=True), (heads, LANES))
                value = jnp.where(lane < 3, top[b], sums)
            rows[piece % 2, pl.ds(b, heads, stride=seqs), :] = value
        value = rows[piece % 2]
        if piece == width // LANES:
            high = value.astype(jnp.bfloat16).astype(jnp.float32)
            middle = (value - high).astype(jnp.bfloat16).astype(jnp.float32)
            low = value - high - middle
            third = lax.broadcasted_iota(jnp.int32, value.shape, 1) % 3
            value = jnp.where(third == 0, high, jnp.where(third == 1, middle, low))
        out_ref[:, :, piece * LANES : (piece + 1) * LANES] = value.reshape(heads, seqs, LANES).astype(jnp.bfloat16)


def combine(width, peers_ref, up_ref, out_ref):
    shards, seqs, _ = peers_ref.shape
    stats = peers_ref[:, :, width:].astype(jnp.float32)
    lane = lax.broadcasted_iota(jnp.int32, stats.shape, 2)
    peak = jnp.sum(jnp.where(lane < 3, stats, 0.0), axis=2, keepdims=True)
    sums = jnp.sum(jnp.where((lane >= 3) & (lane < 6), stats, 0.0), axis=2, keepdims=True)
    rescale = jnp.exp(peak - jnp.max(peak, axis=0, keepdims=True))
    total = jnp.sum(sums * rescale, axis=0)
    mixed = jnp.sum(peers_ref[:, :, :width].astype(jnp.float32) * rescale, axis=0)
    attention = (mixed / total).astype(jnp.bfloat16)
    up = up_ref[...].astype(jnp.float32).reshape(width, up_ref.shape[2]).astype(jnp.bfloat16)
    values = jnp.dot(attention, up, preferred_element_type=jnp.float32).astype(jnp.bfloat16)
    out_ref[...] = jnp.broadcast_to(values[None], out_ref.shape)


def local(
    latent_cache, rope_cache, q_nope, q_rope, w_uk, value_up_weight, w_out, page_table, lengths
):
    slots, page_len, width = latent_cache.shape
    seqs, heads, nope = q_nope.shape
    rope = q_rope.shape[2]
    value_dim = value_up_weight.shape[2]
    cols = w_uk.shape[2]
    shards = lax.axis_size("seq")
    pages = page_table.shape[1]
    scale = (nope + rope) ** -0.5
    f32, bf16 = jnp.float32, jnp.bfloat16

    send_rows = (seqs * heads // LANES + 1) * cols
    sent = pl.pallas_call(
        send_query,
        in_specs=[pl.BlockSpec(memory_space=pltpu.HBM)] * 3,
        out_shape=jax.ShapeDtypeStruct((shards, send_rows, LANES), bf16),
        scratch_shapes=[
            pltpu.VMEM(q_nope.shape, bf16),
            pltpu.VMEM((heads, cols, nope), bf16),
            pltpu.VMEM(value_up_weight.shape, bf16),
            pltpu.SemaphoreType.DMA((3,)),
        ],
        compiler_params=room(8),
    )(hbm(q_nope), hbm(jnp.swapaxes(w_uk, 1, 2)), hbm(value_up_weight))
    recv = lax.all_to_all(sent, "seq", 0, 0, tiled=True)

    first = (lax.axis_index("seq") * slots).astype(jnp.int32).reshape(1)
    most = (slots + seqs * (GROUP - 1)) // GROUP
    most = (most + BATCH - 1) // BATCH * BATCH
    places = (most * GROUP) // slots * slots + slots
    smem = pl.BlockSpec(memory_space=pltpu.SMEM)
    in_hbm = pl.BlockSpec(memory_space=pltpu.HBM)
    order = pl.pallas_call(
        functools.partial(order_slots, page_len),
        out_shape=jax.ShapeDtypeStruct((1, places), jnp.int32),
        in_specs=[smem, smem, in_hbm],
        scratch_shapes=[
            pltpu.VMEM((seqs, pages), jnp.int32),
            pltpu.VMEM((slots, LANES), f32),
            pltpu.VMEM((slots, LANES), f32),
            pltpu.SemaphoreType.DMA,
        ],
        compiler_params=room(4),
    )(first, lengths, hbm(page_table))
    rope_tiles = rope_cache.reshape(slots // 8, 8, page_len * rope // LANES, LANES)
    rope_tiles = jnp.swapaxes(rope_tiles, 1, 2)
    tokens = GROUP * page_len
    rope_score = pl.pallas_call(
        functools.partial(score_rope, scale, page_len),
        out_shape=pltpu.HBM((most, heads, tokens), f32),
        in_specs=[smem, in_hbm, in_hbm],
        scratch_shapes=[
            pltpu.VMEM(q_rope.shape, bf16),
            pltpu.VMEM(rope_tiles.shape, bf16),
            pltpu.VMEM((page_len * rope * 8 // LANES, LANES), f32),
            pltpu.VMEM((8, page_len, LANES), f32),
            pltpu.VMEM((slots, page_len, LANES), bf16),
            pltpu.SemaphoreType.DMA((2,)),
        ],
        compiler_params=room(16),
    )(order, hbm(q_rope), hbm(rope_tiles))

    out_width = width + LANES
    partial, up = pl.pallas_call(
        functools.partial(attend, scale, page_len),
        out_shape=(
            jax.ShapeDtypeStruct((heads, seqs, out_width), bf16),
            jax.ShapeDtypeStruct((shards, cols, LANES), bf16),
        ),
        in_specs=[
            smem,
            whole(recv.shape),
            in_hbm,
            in_hbm,
        ],
        scratch_shapes=[
            pltpu.VMEM((most, tokens, width), bf16),
            pltpu.VMEM((seqs * heads, width), bf16),
            pltpu.VMEM((most, heads, tokens), f32),
            pltpu.VMEM((seqs, heads, LANES), f32),
            pltpu.VMEM((seqs, heads, LANES), f32),
            pltpu.VMEM((seqs, heads, width), f32),
            pltpu.VMEM((2, seqs * heads, LANES), f32),
            pltpu.SemaphoreType.DMA((most // BATCH,)),
            pltpu.SemaphoreType.DMA((most // BATCH,)),
        ],
        compiler_params=room(24),
    )(order, recv, hbm(rope_score), hbm(latent_cache))
    peers = lax.all_to_all(partial, "seq", 0, 0, tiled=True)

    values = pl.pallas_call(
        functools.partial(combine, width),
        out_shape=jax.ShapeDtypeStruct((shards, seqs, value_dim), bf16),
        compiler_params=room(8),
    )(peers, up)
    every = lax.all_to_all(values, "seq", 0, 0, tiled=True)
    flat = jnp.swapaxes(every, 0, 1).reshape(seqs, heads * value_dim)
    half = jnp.dot(flat, w_out, preferred_element_type=f32)
    both = half + lax.ppermute(half, "mp", [(0, 1), (1, 0)])
    share = half.shape[1] // lax.axis_size("mp")
    return lax.dynamic_slice_in_dim(both, lax.axis_index("mp") * share, share, 1).astype(bf16)


def solution(mesh):
    return jax.shard_map(
        local,
        mesh=mesh,
        in_specs=(
            P(("groups", "seq"), None, None),
            P(("groups", "seq"), None),
            P("groups", "mp", None),
            P("groups", "mp", None),
            P("mp", None, "seq"),
            P("mp", "seq", None),
            P("mp", "seq"),
            P("groups", None),
            P("groups"),
        ),
        out_specs=P("groups", ("seq", "mp")),
        check_vma=False,
    )
```

```python
import functools

import jax
import jax.numpy as jnp
from jax import lax
from jax.experimental import pallas as pl
from jax.experimental.pallas import tpu as pltpu
from jax.sharding import Mesh
from jax.sharding import PartitionSpec as P

NEG = -1e30
LANES = 128
GROUP = 4
BATCH = 4
NT = (((1,), (1,)), ((), ()))


def whole(shape):
    return pl.BlockSpec(shape, lambda *_: (0,) * len(shape))


def room(mib):
    return pltpu.CompilerParams(vmem_limit_bytes=mib * 1024 * 1024)


def hbm(x):
    return pltpu.with_memory_space_constraint(x, pltpu.HBM)


def send_query(q_hbm, w_hbm, v_hbm, out_ref, q_ref, w_ref, v_ref, sems):
    seqs, heads, nope = q_ref.shape
    cols = w_ref.shape[1]
    moves = [
        pltpu.make_async_copy(source, target, sems.at[i])
        for i, (source, target) in enumerate(((q_hbm, q_ref), (w_hbm, w_ref), (v_hbm, v_ref)))
    ]
    for move in moves:
        move.start()
    for move in moves:
        move.wait()
    q = q_ref[...].reshape(seqs * heads, nope)
    w = w_ref[...].reshape(heads * cols, nope)
    every = lax.dot_general(w, q, NT, preferred_element_type=jnp.float32)
    every = every.reshape(heads, cols, seqs * heads)
    head = lax.broadcasted_iota(jnp.int32, every.shape, 0)
    lane = lax.broadcasted_iota(jnp.int32, every.shape, 2)
    part = jnp.sum(jnp.where(lane % heads == head, every, 0.0), axis=0).astype(jnp.bfloat16)
    shards = out_ref.shape[0]
    tiles = seqs * heads // LANES
    for tile in range(tiles):
        piece = part[:, tile * LANES : (tile + 1) * LANES]
        out_ref[:, tile * cols : (tile + 1) * cols, :] = jnp.broadcast_to(piece[None], (shards, cols, LANES))
    out_ref[:, tiles * cols :, :] = v_ref[...]


def order_slots(page_len, first_ref, lengths_ref, table_hbm, out_ref, table_ref, owner_sum, fill_sum, sem):
    seqs, pages = table_ref.shape
    slots = owner_sum.shape[0]
    places = out_ref.shape[1]
    f32, bf16 = jnp.float32, jnp.bfloat16
    logical = lax.broadcasted_iota(jnp.int32, (seqs, pages), 1)
    seq = lax.broadcasted_iota(jnp.int32, (seqs, pages), 0)
    move = pltpu.make_async_copy(table_hbm, table_ref, sem)
    move.start()
    length = jnp.zeros((seqs, pages), jnp.int32)
    for b in range(seqs):
        length = jnp.where(seq == b, lengths_ref[b], length)
    left = length - page_len * logical
    move.wait()
    local_slot = jnp.where(left > 0, table_ref[...] - first_ref[0], -1)
    tokens = jnp.clip(left, 0, page_len)
    code = (seq * LANES + tokens).astype(f32)

    def at_slot(slot, carry):
        hit = jnp.where(local_slot == slot, code, 0.0)
        acc = hit[:, :LANES]
        for j in range(1, pages // LANES):
            acc = acc + hit[:, j * LANES : (j + 1) * LANES]
        row = jnp.sum(acc, axis=0, keepdims=True)
        owner = jnp.floor(row * (1.0 / LANES))
        owner_sum[pl.ds(slot, 1), :] = owner
        fill_sum[pl.ds(slot, 1), :] = row - owner * LANES
        return carry

    lax.fori_loop(0, slots, at_slot, 0, unroll=4)
    ones = jnp.ones((8, LANES), bf16)
    owner = lax.dot_general(ones, owner_sum[...].astype(bf16), NT, preferred_element_type=f32)
    fill = lax.dot_general(ones, fill_sum[...].astype(bf16), NT, preferred_element_type=f32)

    row = lax.broadcasted_iota(jnp.int32, (seqs, slots), 0)
    slot = lax.broadcasted_iota(jnp.int32, (seqs, slots), 1)
    mine = (owner[:seqs] == row.astype(f32)) & (fill[:seqs] > 0.0)
    ours = jnp.where(mine, 1.0, 0.0)
    before = lax.broadcasted_iota(jnp.int32, (slots, slots), 0) < lax.broadcasted_iota(
        jnp.int32, (slots, slots), 1
    )
    rank = jnp.dot(ours.astype(bf16), jnp.where(before, 1.0, 0.0).astype(bf16), preferred_element_type=f32)
    count = jnp.broadcast_to(jnp.sum(ours, axis=1, keepdims=True), (seqs, slots))
    groups = jnp.floor((count + (GROUP - 1)) * (1.0 / GROUP))
    base, starts = jnp.zeros((1, slots), f32), []
    for b in range(seqs):
        starts.append(base)
        base = base + groups[b : b + 1]
    place = GROUP * jnp.concatenate(starts, axis=0) + rank
    place = jnp.sum(jnp.where(mine, place + 1.0, 0.0), axis=0, keepdims=True) - 1.0
    at = lax.broadcasted_iota(jnp.int32, (places, slots), 0).astype(f32) == place
    value = jnp.where(row == 0, slot.astype(f32), jnp.where(row == 1, fill[:seqs], owner[:seqs]))
    found = lax.dot_general(
        value.astype(bf16), jnp.where(at, 1.0, 0.0).astype(bf16), NT, preferred_element_type=f32
    )
    packed = (found[2:3] * LANES + found[0:1]) * LANES + found[1:2]
    place = lax.broadcasted_iota(jnp.int32, (1, places), 1)
    total = jnp.concatenate([base] * (places // slots), axis=1)
    out_ref[...] = jnp.where(place == places - 1, total, packed).astype(jnp.int32)


SHIFT = 7


def steps_of(order_ref, batch):
    return (order_ref[0, order_ref.shape[1] - 1] + (batch - 1)) // batch


def slot_at(order_ref, group, k):
    code = order_ref[0, GROUP * group + k]
    return lax.shift_right_logical(code, SHIFT) & (LANES - 1), code & (LANES - 1)


def owner_of(order_ref, group):
    return lax.shift_right_logical(order_ref[0, GROUP * group], 2 * SHIFT)


def score_rope(
    scale, page_len, order_ref, q_hbm, tiles_hbm, out_ref, q_ref, tiles, flat, spread, keys, sems
):
    heads, rope = q_ref.shape[1:]
    blocks, pairs, _, _ = tiles.shape
    first = pltpu.make_async_copy(q_hbm, q_ref, sems.at[0])
    second = pltpu.make_async_copy(tiles_hbm, tiles, sems.at[1])
    first.start()
    second.start()
    first.wait()
    second.wait()
    even = lax.broadcasted_iota(jnp.int32, (pairs, LANES), 1) < rope

    def spread_block(block, carry):
        flat[...] = tiles[block].astype(jnp.float32).reshape(pairs * 8, LANES)
        for k in range(8):
            two = flat[pl.ds(k, pairs, stride=8), :]
            spread[k, pl.ds(0, pairs, stride=2), :] = jnp.where(even, two, 0.0)
            spread[k, pl.ds(1, pairs, stride=2), :] = jnp.where(even, 0.0, two)
        keys[pl.ds(block * 8, 8)] = spread[...].astype(jnp.bfloat16)
        return carry

    lax.fori_loop(0, blocks, spread_block, 0)
    lane = lax.broadcasted_iota(jnp.int32, (heads, GROUP * page_len), 1)

    def score(step, carry):
        for j in range(BATCH):
            group = step * BATCH + j
            rows, limit = [], None
            for k in range(GROUP):
                slot, fill = slot_at(order_ref, group, k)
                rows.append(keys[slot])
                end = k * page_len + fill
                limit = end if limit is None else jnp.where(lane >= k * page_len, end, limit)
            query = q_ref[owner_of(order_ref, group)].astype(jnp.float32)
            query = jnp.concatenate([query, query], axis=1).astype(jnp.bfloat16)
            both = lax.dot_general(
                query, jnp.concatenate(rows, axis=0), NT, preferred_element_type=jnp.float32
            )
            out_ref[group] = jnp.where(lane < limit, both * scale, NEG)
        return carry

    lax.fori_loop(0, steps_of(order_ref, BATCH), score, 0)


def attend(
    scale, page_len, sender, order_ref, recv_ref, rope_hbm, latent_hbm, out_ref, up_ref,
    latent, query, scores, top, total, acc, rows, sems, rope_sems,
):
    _, tokens, width = latent.shape
    seqs, heads, _ = top.shape
    steps = steps_of(order_ref, BATCH)

    def fetch(step):
        for j in range(BATCH):
            group = step * BATCH + j
            for k in range(GROUP):
                slot, _ = slot_at(order_ref, group, k)
                pltpu.make_async_copy(
                    latent_hbm.at[slot], latent.at[group, pl.ds(k * page_len, page_len)], sems.at[step]
                ).start()
        batch = pl.ds(step * BATCH, BATCH)
        pltpu.make_async_copy(rope_hbm.at[batch], scores.at[batch], rope_sems.at[step]).start()

    ahead = 3
    for step in range(ahead):

        @pl.when(step < steps)
        def _():
            fetch(step)

    cols = recv_ref.shape[1] // (seqs * heads // LANES + 1)
    for tile in range(seqs * heads // LANES):
        block = recv_ref[:, tile * cols : (tile + 1) * cols, :].astype(jnp.float32)
        block = jnp.concatenate([block[at] for at in sender], axis=0)
        query[tile * LANES : (tile + 1) * LANES, :] = block.T.astype(jnp.bfloat16)
    for shard, at in enumerate(sender):
        up_ref[shard] = recv_ref[at, recv_ref.shape[1] - cols :, :]
    top[...] = jnp.full(top.shape, NEG, jnp.float32)
    total[...] = jnp.zeros(total.shape, jnp.float32)
    acc[...] = jnp.zeros(acc.shape, jnp.float32)

    def score(step, carry):
        @pl.when(step + ahead < steps)
        def _():
            fetch(step + ahead)

        batch = pl.ds(step * BATCH, BATCH)
        pltpu.make_async_copy(latent.at[batch], latent.at[batch], sems.at[step]).wait()
        pltpu.make_async_copy(rope_hbm.at[batch], scores.at[batch], rope_sems.at[step]).wait()
        made = []
        for j in range(BATCH):
            group = step * BATCH + j
            b = owner_of(order_ref, group)
            lhs = query[pl.ds(pl.multiple_of(b * heads, heads), heads), :]
            both = lax.dot_general(lhs, latent[group], NT, preferred_element_type=jnp.float32)
            made.append((group, b, both * scale + scores[group]))
        for group, b, both in made:
            scores[group] = both
            high = both[:, :LANES]
            for k in range(1, tokens // LANES):
                high = jnp.maximum(high, both[:, k * LANES : (k + 1) * LANES])
            top[b] = jnp.maximum(top[b], high)
        return carry

    lax.fori_loop(0, steps, score, 0)

    for b in range(seqs):
        top[b] = jnp.broadcast_to(jnp.max(top[b], axis=1, keepdims=True), (heads, LANES))

    def weigh(step, carry):
        made = []
        for j in range(BATCH):
            group = step * BATCH + j
            b = owner_of(order_ref, group)
            both = scores[group]
            peak = top[b]
            parts, some = [], None
            for k in range(tokens // LANES):
                part = both[:, k * LANES : (k + 1) * LANES]
                part = jnp.where(part > 0.5 * NEG, jnp.exp(part - peak), 0.0)
                some = part if some is None else some + part
                parts.append(part.astype(jnp.bfloat16))
            lhs = jnp.concatenate(parts, axis=1)
            made.append((b, some, jnp.dot(lhs, latent[group], preferred_element_type=jnp.float32)))
        for b, some, out in made:
            total[b] = total[b] + some
            acc[b] = acc[b] + out
        return carry

    lax.fori_loop(0, steps, weigh, 0)

    lane = lax.broadcasted_iota(jnp.int32, (heads, LANES), 1)
    for piece in range(width // LANES + 1):
        for b in range(seqs):
            if piece < width // LANES:
                value = acc[b, :, piece * LANES : (piece + 1) * LANES]
            else:
                sums = jnp.broadcast_to(jnp.sum(total[b], axis=1, keepdims=True), (heads, LANES))
                value = jnp.where(lane < 3, top[b], sums)
            rows[piece % 2, pl.ds(b, heads, stride=seqs), :] = value
        value = rows[piece % 2]
        if piece == width // LANES:
            high = value.astype(jnp.bfloat16).astype(jnp.float32)
            middle = (value - high).astype(jnp.bfloat16).astype(jnp.float32)
            low = value - high - middle
            third = lax.broadcasted_iota(jnp.int32, value.shape, 1) % 3
            value = jnp.where(third == 0, high, jnp.where(third == 1, middle, low))
        out_ref[:, :, piece * LANES : (piece + 1) * LANES] = value.reshape(heads, seqs, LANES).astype(jnp.bfloat16)


def combine(width, peers_ref, up_ref, out_ref):
    shards, seqs, _ = peers_ref.shape
    stats = peers_ref[:, :, width:].astype(jnp.float32)
    lane = lax.broadcasted_iota(jnp.int32, stats.shape, 2)
    peak = jnp.sum(jnp.where(lane < 3, stats, 0.0), axis=2, keepdims=True)
    sums = jnp.sum(jnp.where((lane >= 3) & (lane < 6), stats, 0.0), axis=2, keepdims=True)
    rescale = jnp.exp(peak - jnp.max(peak, axis=0, keepdims=True))
    total = jnp.sum(sums * rescale, axis=0)
    mixed = jnp.sum(peers_ref[:, :, :width].astype(jnp.float32) * rescale, axis=0)
    attention = (mixed / total).astype(jnp.bfloat16)
    up = up_ref[...].astype(jnp.float32).reshape(width, up_ref.shape[2]).astype(jnp.bfloat16)
    values = jnp.dot(attention, up, preferred_element_type=jnp.float32).astype(jnp.bfloat16)
    out_ref[...] = jnp.broadcast_to(values[None], out_ref.shape)


def local(
    seq, peers_order,
    latent_cache, rope_cache, q_nope, q_rope, w_uk, value_up_weight, w_out, page_table, lengths,
):
    slots, page_len, width = latent_cache.shape
    seqs, heads, nope = q_nope.shape
    rope = q_rope.shape[2]
    value_dim = value_up_weight.shape[2]
    cols = w_uk.shape[2]
    shards = lax.axis_size(seq)
    pages = page_table.shape[1]
    scale = (nope + rope) ** -0.5
    f32, bf16 = jnp.float32, jnp.bfloat16

    send_rows = (seqs * heads // LANES + 1) * cols
    sent = pl.pallas_call(
        send_query,
        in_specs=[pl.BlockSpec(memory_space=pltpu.HBM)] * 3,
        out_shape=jax.ShapeDtypeStruct((shards, send_rows, LANES), bf16),
        scratch_shapes=[
            pltpu.VMEM(q_nope.shape, bf16),
            pltpu.VMEM((heads, cols, nope), bf16),
            pltpu.VMEM(value_up_weight.shape, bf16),
            pltpu.SemaphoreType.DMA((3,)),
        ],
        compiler_params=room(8),
    )(hbm(q_nope), hbm(jnp.swapaxes(w_uk, 1, 2)), hbm(value_up_weight))
    recv = lax.all_to_all(sent, peers_order, 0, 0, tiled=True)

    first = (lax.axis_index(seq) * slots).astype(jnp.int32).reshape(1)
    most = (slots + seqs * (GROUP - 1)) // GROUP
    most = (most + BATCH - 1) // BATCH * BATCH
    places = (most * GROUP) // slots * slots + slots
    smem = pl.BlockSpec(memory_space=pltpu.SMEM)
    in_hbm = pl.BlockSpec(memory_space=pltpu.HBM)
    order = pl.pallas_call(
        functools.partial(order_slots, page_len),
        out_shape=jax.ShapeDtypeStruct((1, places), jnp.int32),
        in_specs=[smem, smem, in_hbm],
        scratch_shapes=[
            pltpu.VMEM((seqs, pages), jnp.int32),
            pltpu.VMEM((slots, LANES), f32),
            pltpu.VMEM((slots, LANES), f32),
            pltpu.SemaphoreType.DMA,
        ],
        compiler_params=room(4),
    )(first, lengths, hbm(page_table))
    rope_tiles = rope_cache.reshape(slots // 8, 8, page_len * rope // LANES, LANES)
    rope_tiles = jnp.swapaxes(rope_tiles, 1, 2)
    tokens = GROUP * page_len
    rope_score = pl.pallas_call(
        functools.partial(score_rope, scale, page_len),
        out_shape=pltpu.HBM((most, heads, tokens), f32),
        in_specs=[smem, in_hbm, in_hbm],
        scratch_shapes=[
            pltpu.VMEM(q_rope.shape, bf16),
            pltpu.VMEM(rope_tiles.shape, bf16),
            pltpu.VMEM((page_len * rope * 8 // LANES, LANES), f32),
            pltpu.VMEM((8, page_len, LANES), f32),
            pltpu.VMEM((slots, page_len, LANES), bf16),
            pltpu.SemaphoreType.DMA((2,)),
        ],
        compiler_params=room(16),
    )(order, hbm(q_rope), hbm(rope_tiles))

    out_width = width + LANES
    partial, up = pl.pallas_call(
        functools.partial(attend, scale, page_len, sender_of(seq, peers_order)),
        out_shape=(
            jax.ShapeDtypeStruct((heads, seqs, out_width), bf16),
            jax.ShapeDtypeStruct((shards, cols, LANES), bf16),
        ),
        in_specs=[
            smem,
            whole(recv.shape),
            in_hbm,
            in_hbm,
        ],
        scratch_shapes=[
            pltpu.VMEM((most, tokens, width), bf16),
            pltpu.VMEM((seqs * heads, width), bf16),
            pltpu.VMEM((most, heads, tokens), f32),
            pltpu.VMEM((seqs, heads, LANES), f32),
            pltpu.VMEM((seqs, heads, LANES), f32),
            pltpu.VMEM((seqs, heads, width), f32),
            pltpu.VMEM((2, seqs * heads, LANES), f32),
            pltpu.SemaphoreType.DMA((most // BATCH,)),
            pltpu.SemaphoreType.DMA((most // BATCH,)),
        ],
        compiler_params=room(24),
    )(order, recv, hbm(rope_score), hbm(latent_cache))
    peers = lax.all_to_all(partial, peers_order, 0, 0, tiled=True)

    values = pl.pallas_call(
        functools.partial(combine, width),
        out_shape=jax.ShapeDtypeStruct((shards, seqs, value_dim), bf16),
        compiler_params=room(8),
    )(peers, up)
    every = lax.all_to_all(values, peers_order, 0, 0, tiled=True)
    flat = jnp.swapaxes(every, 0, 1).reshape(seqs, heads * value_dim)
    half = jnp.dot(flat, w_out, preferred_element_type=f32)
    both = half + lax.ppermute(half, "mp", [(0, 1), (1, 0)])
    share = half.shape[1] // lax.axis_size("mp")
    return lax.dynamic_slice_in_dim(both, lax.axis_index("mp") * share, share, 1).astype(bf16)


def sender_of(seq, peers_order):
    bits = len(seq)
    places = []
    for shard in range(2**bits):
        bit = {axis: shard >> (bits - 1 - i) & 1 for i, axis in enumerate(seq)}
        places.append(sum(bit[axis] << (bits - 1 - i) for i, axis in enumerate(peers_order)))
    return tuple(places)


def solution(mesh):
    bits = mesh.shape["seq"].bit_length() - 1
    assert mesh.shape["seq"] == 2**bits and bits % 2 == 0
    seq = tuple(f"seq_{i}" for i in range(bits))
    peers_order = tuple(axis for both in zip(seq[: bits // 2], seq[bits // 2 :]) for axis in both)
    finer = Mesh(
        mesh.devices.reshape(mesh.shape["groups"], *(2,) * bits, mesh.shape["mp"]),
        ("groups", *seq, "mp"),
    )
    return jax.shard_map(
        functools.partial(local, seq, peers_order),
        mesh=finer,
        in_specs=(
            P(("groups", *seq), None, None),
            P(("groups", *seq), None),
            P("groups", "mp", None),
            P("groups", "mp", None),
            P("mp", None, seq),
            P("mp", seq, None),
            P("mp", seq),
            P("groups", None),
            P("groups"),
        ),
        out_specs=P("groups", (*seq, "mp")),
        check_vma=False,
    )
```

```python
import functools

import jax
import jax.numpy as jnp
from jax import lax
from jax.experimental import pallas as pl
from jax.experimental.pallas import tpu as pltpu
from jax.sharding import Mesh
from jax.sharding import PartitionSpec as P

NEG = -1e30
LANES = 128
GROUP = 4
BATCH = 4
NT = (((1,), (1,)), ((), ()))


def whole(shape):
    return pl.BlockSpec(shape, lambda *_: (0,) * len(shape))


def room(mib):
    return pltpu.CompilerParams(vmem_limit_bytes=mib * 1024 * 1024)


def hbm(x):
    return pltpu.with_memory_space_constraint(x, pltpu.HBM)


def send_query(q_hbm, w_hbm, v_hbm, out_ref, q_ref, w_ref, v_ref, sems):
    seqs, heads, nope = q_ref.shape
    cols = w_ref.shape[1]
    moves = [
        pltpu.make_async_copy(source, target, sems.at[i])
        for i, (source, target) in enumerate(((q_hbm, q_ref), (w_hbm, w_ref), (v_hbm, v_ref)))
    ]
    for move in moves:
        move.start()
    for move in moves:
        move.wait()
    q = q_ref[...].reshape(seqs * heads, nope)
    w = w_ref[...].reshape(heads * cols, nope)
    every = lax.dot_general(w, q, NT, preferred_element_type=jnp.float32)
    every = every.reshape(heads, cols, seqs * heads)
    head = lax.broadcasted_iota(jnp.int32, every.shape, 0)
    lane = lax.broadcasted_iota(jnp.int32, every.shape, 2)
    part = jnp.sum(jnp.where(lane % heads == head, every, 0.0), axis=0).astype(jnp.bfloat16)
    shards = out_ref.shape[0]
    tiles = seqs * heads // LANES
    for tile in range(tiles):
        piece = part[:, tile * LANES : (tile + 1) * LANES]
        out_ref[:, tile * cols : (tile + 1) * cols, :] = jnp.broadcast_to(piece[None], (shards, cols, LANES))
    out_ref[:, tiles * cols :, :] = v_ref[...]


def order_slots(page_len, first_ref, lengths_ref, table_hbm, out_ref, table_ref, owner_sum, fill_sum, sem):
    seqs, pages = table_ref.shape
    slots = owner_sum.shape[0]
    places = out_ref.shape[1]
    f32, bf16 = jnp.float32, jnp.bfloat16
    logical = lax.broadcasted_iota(jnp.int32, (seqs, pages), 1)
    seq = lax.broadcasted_iota(jnp.int32, (seqs, pages), 0)
    move = pltpu.make_async_copy(table_hbm, table_ref, sem)
    move.start()
    length = jnp.zeros((seqs, pages), jnp.int32)
    for b in range(seqs):
        length = jnp.where(seq == b, lengths_ref[b], length)
    left = length - page_len * logical
    move.wait()
    local_slot = jnp.where(left > 0, table_ref[...] - first_ref[0], -1)
    tokens = jnp.clip(left, 0, page_len)
    code = (seq * LANES + tokens).astype(f32)

    def at_slot(slot, carry):
        hit = jnp.where(local_slot == slot, code, 0.0)
        acc = hit[:, :LANES]
        for j in range(1, pages // LANES):
            acc = acc + hit[:, j * LANES : (j + 1) * LANES]
        row = jnp.sum(acc, axis=0, keepdims=True)
        owner = jnp.floor(row * (1.0 / LANES))
        owner_sum[pl.ds(slot, 1), :] = owner
        fill_sum[pl.ds(slot, 1), :] = row - owner * LANES
        return carry

    lax.fori_loop(0, slots, at_slot, 0, unroll=4)
    ones = jnp.ones((8, LANES), bf16)
    owner = lax.dot_general(ones, owner_sum[...].astype(bf16), NT, preferred_element_type=f32)
    fill = lax.dot_general(ones, fill_sum[...].astype(bf16), NT, preferred_element_type=f32)

    row = lax.broadcasted_iota(jnp.int32, (seqs, slots), 0)
    slot = lax.broadcasted_iota(jnp.int32, (seqs, slots), 1)
    mine = (owner[:seqs] == row.astype(f32)) & (fill[:seqs] > 0.0)
    ours = jnp.where(mine, 1.0, 0.0)
    before = lax.broadcasted_iota(jnp.int32, (slots, slots), 0) < lax.broadcasted_iota(
        jnp.int32, (slots, slots), 1
    )
    rank = jnp.dot(ours.astype(bf16), jnp.where(before, 1.0, 0.0).astype(bf16), preferred_element_type=f32)
    count = jnp.broadcast_to(jnp.sum(ours, axis=1, keepdims=True), (seqs, slots))
    groups = jnp.floor((count + (GROUP - 1)) * (1.0 / GROUP))
    base, starts = jnp.zeros((1, slots), f32), []
    for b in range(seqs):
        starts.append(base)
        base = base + groups[b : b + 1]
    place = GROUP * jnp.concatenate(starts, axis=0) + rank
    place = jnp.sum(jnp.where(mine, place + 1.0, 0.0), axis=0, keepdims=True) - 1.0
    at = lax.broadcasted_iota(jnp.int32, (places, slots), 0).astype(f32) == place
    value = jnp.where(row == 0, slot.astype(f32), jnp.where(row == 1, fill[:seqs], owner[:seqs]))
    found = lax.dot_general(
        value.astype(bf16), jnp.where(at, 1.0, 0.0).astype(bf16), NT, preferred_element_type=f32
    )
    packed = (found[2:3] * LANES + found[0:1]) * LANES + found[1:2]
    place = lax.broadcasted_iota(jnp.int32, (1, places), 1)
    total = jnp.concatenate([base] * (places // slots), axis=1)
    out_ref[...] = jnp.where(place == places - 1, total, packed).astype(jnp.int32)


SHIFT = 7


def steps_of(order_ref, batch):
    return (order_ref[0, order_ref.shape[1] - 1] + (batch - 1)) // batch


def slot_at(order_ref, group, k):
    code = order_ref[0, GROUP * group + k]
    return lax.shift_right_logical(code, SHIFT) & (LANES - 1), code & (LANES - 1)


def owner_of(order_ref, group):
    return lax.shift_right_logical(order_ref[0, GROUP * group], 2 * SHIFT)


def score_rope(
    scale, page_len, order_ref, q_hbm, tiles_hbm, out_ref, q_ref, tiles, flat, spread, keys, sems
):
    heads, rope = q_ref.shape[1:]
    blocks, pairs, _, _ = tiles.shape
    first = pltpu.make_async_copy(q_hbm, q_ref, sems.at[0])
    second = pltpu.make_async_copy(tiles_hbm, tiles, sems.at[1])
    first.start()
    second.start()
    first.wait()
    second.wait()
    even = lax.broadcasted_iota(jnp.int32, (pairs, LANES), 1) < rope

    def spread_block(block, carry):
        flat[...] = tiles[block].astype(jnp.float32).reshape(pairs * 8, LANES)
        for k in range(8):
            two = flat[pl.ds(k, pairs, stride=8), :]
            spread[k, pl.ds(0, pairs, stride=2), :] = jnp.where(even, two, 0.0)
            spread[k, pl.ds(1, pairs, stride=2), :] = jnp.where(even, 0.0, two)
        keys[pl.ds(block * 8, 8)] = spread[...].astype(jnp.bfloat16)
        return carry

    lax.fori_loop(0, blocks, spread_block, 0)
    lane = lax.broadcasted_iota(jnp.int32, (heads, GROUP * page_len), 1)

    def score(step, carry):
        for j in range(BATCH):
            group = step * BATCH + j
            rows, limit = [], None
            for k in range(GROUP):
                slot, fill = slot_at(order_ref, group, k)
                rows.append(keys[slot])
                end = k * page_len + fill
                limit = end if limit is None else jnp.where(lane >= k * page_len, end, limit)
            query = q_ref[owner_of(order_ref, group)].astype(jnp.float32)
            query = jnp.concatenate([query, query], axis=1).astype(jnp.bfloat16)
            both = lax.dot_general(
                query, jnp.concatenate(rows, axis=0), NT, preferred_element_type=jnp.float32
            )
            out_ref[group] = jnp.where(lane < limit, both * scale, NEG)
        return carry

    lax.fori_loop(0, steps_of(order_ref, BATCH), score, 0)


def attend(
    scale, page_len, sender, order_ref, recv_ref, rope_hbm, latent_hbm, out_ref, up_ref,
    latent, query, scores, top, total, acc, rows, sems, rope_sems,
):
    _, tokens, width = latent.shape
    seqs, heads, _ = top.shape
    steps = steps_of(order_ref, BATCH)

    def fetch(step):
        for j in range(BATCH):
            group = step * BATCH + j
            for k in range(GROUP):
                slot, _ = slot_at(order_ref, group, k)
                pltpu.make_async_copy(
                    latent_hbm.at[slot], latent.at[group, pl.ds(k * page_len, page_len)], sems.at[step]
                ).start()
        batch = pl.ds(step * BATCH, BATCH)
        pltpu.make_async_copy(rope_hbm.at[batch], scores.at[batch], rope_sems.at[step]).start()

    ahead = 3
    for step in range(ahead):

        @pl.when(step < steps)
        def _():
            fetch(step)

    cols = recv_ref.shape[1] // (seqs * heads // LANES + 1)
    for tile in range(seqs * heads // LANES):
        block = recv_ref[:, tile * cols : (tile + 1) * cols, :].astype(jnp.float32)
        block = jnp.concatenate([block[at] for at in sender], axis=0)
        query[tile * LANES : (tile + 1) * LANES, :] = block.T.astype(jnp.bfloat16)
    for shard, at in enumerate(sender):
        up_ref[shard] = recv_ref[at, recv_ref.shape[1] - cols :, :]
    top[...] = jnp.full(top.shape, NEG, jnp.float32)
    total[...] = jnp.zeros(total.shape, jnp.float32)
    acc[...] = jnp.zeros(acc.shape, jnp.float32)

    def score(step, carry):
        @pl.when(step + ahead < steps)
        def _():
            fetch(step + ahead)

        batch = pl.ds(step * BATCH, BATCH)
        pltpu.make_async_copy(latent.at[batch], latent.at[batch], sems.at[step]).wait()
        pltpu.make_async_copy(rope_hbm.at[batch], scores.at[batch], rope_sems.at[step]).wait()
        made = []
        for j in range(BATCH):
            group = step * BATCH + j
            b = owner_of(order_ref, group)
            lhs = query[pl.ds(pl.multiple_of(b * heads, heads), heads), :]
            both = lax.dot_general(lhs, latent[group], NT, preferred_element_type=jnp.float32)
            made.append((group, b, both * scale + scores[group]))
        for group, b, both in made:
            scores[group] = both
            high = both[:, :LANES]
            for k in range(1, tokens // LANES):
                high = jnp.maximum(high, both[:, k * LANES : (k + 1) * LANES])
            top[b] = jnp.maximum(top[b], high)
        return carry

    lax.fori_loop(0, steps, score, 0)

    for b in range(seqs):
        top[b] = jnp.broadcast_to(jnp.max(top[b], axis=1, keepdims=True), (heads, LANES))

    def weigh(step, carry):
        made = []
        for j in range(BATCH):
            group = step * BATCH + j
            b = owner_of(order_ref, group)
            both = scores[group]
            peak = top[b]
            parts, some = [], None
            for k in range(tokens // LANES):
                part = both[:, k * LANES : (k + 1) * LANES]
                part = jnp.where(part > 0.5 * NEG, jnp.exp(part - peak), 0.0)
                some = part if some is None else some + part
                parts.append(part.astype(jnp.bfloat16))
            lhs = jnp.concatenate(parts, axis=1)
            made.append((b, some, jnp.dot(lhs, latent[group], preferred_element_type=jnp.float32)))
        for b, some, out in made:
            total[b] = total[b] + some
            acc[b] = acc[b] + out
        return carry

    lax.fori_loop(0, steps, weigh, 0)

    lane = lax.broadcasted_iota(jnp.int32, (heads, LANES), 1)
    for piece in range(width // LANES + 1):
        for b in range(seqs):
            if piece < width // LANES:
                value = acc[b, :, piece * LANES : (piece + 1) * LANES]
            else:
                sums = jnp.broadcast_to(jnp.sum(total[b], axis=1, keepdims=True), (heads, LANES))
                value = jnp.where(lane < 3, top[b], sums)
            rows[piece % 2, pl.ds(b, heads, stride=seqs), :] = value
        value = rows[piece % 2]
        if piece == width // LANES:
            high = value.astype(jnp.bfloat16).astype(jnp.float32)
            middle = (value - high).astype(jnp.bfloat16).astype(jnp.float32)
            low = value - high - middle
            third = lax.broadcasted_iota(jnp.int32, value.shape, 1) % 3
            value = jnp.where(third == 0, high, jnp.where(third == 1, middle, low))
        out_ref[:, :, piece * LANES : (piece + 1) * LANES] = value.reshape(heads, seqs, LANES).astype(jnp.bfloat16)


def combine(width, peers_ref, up_ref, out_ref):
    shards, seqs, _ = peers_ref.shape
    stats = peers_ref[:, :, width:].astype(jnp.float32)
    lane = lax.broadcasted_iota(jnp.int32, stats.shape, 2)
    peak = jnp.sum(jnp.where(lane < 3, stats, 0.0), axis=2, keepdims=True)
    sums = jnp.sum(jnp.where((lane >= 3) & (lane < 6), stats, 0.0), axis=2, keepdims=True)
    rescale = jnp.exp(peak - jnp.max(peak, axis=0, keepdims=True))
    total = jnp.sum(sums * rescale, axis=0)
    mixed = jnp.sum(peers_ref[:, :, :width].astype(jnp.float32) * rescale, axis=0)
    attention = (mixed / total).astype(jnp.bfloat16)
    up = up_ref[...].astype(jnp.float32).reshape(width, up_ref.shape[2]).astype(jnp.bfloat16)
    values = jnp.dot(attention, up, preferred_element_type=jnp.float32).astype(jnp.bfloat16)
    out_ref[...] = jnp.broadcast_to(values[None], out_ref.shape)


def local(
    seq, peers_order,
    latent_cache, rope_cache, q_nope, q_rope, w_uk, value_up_weight, w_out, page_table, lengths,
):
    slots, page_len, width = latent_cache.shape
    seqs, heads, nope = q_nope.shape
    rope = q_rope.shape[2]
    value_dim = value_up_weight.shape[2]
    cols = w_uk.shape[2]
    shards = lax.axis_size(seq)
    pages = page_table.shape[1]
    scale = (nope + rope) ** -0.5
    f32, bf16 = jnp.float32, jnp.bfloat16

    send_rows = (seqs * heads // LANES + 1) * cols
    sent = pl.pallas_call(
        send_query,
        in_specs=[pl.BlockSpec(memory_space=pltpu.HBM)] * 3,
        out_shape=jax.ShapeDtypeStruct((shards, send_rows, LANES), bf16),
        scratch_shapes=[
            pltpu.VMEM(q_nope.shape, bf16),
            pltpu.VMEM((heads, cols, nope), bf16),
            pltpu.VMEM(value_up_weight.shape, bf16),
            pltpu.SemaphoreType.DMA((3,)),
        ],
        compiler_params=room(8),
    )(hbm(q_nope), hbm(jnp.swapaxes(w_uk, 1, 2)), hbm(value_up_weight))
    recv = lax.all_to_all(sent, peers_order, 0, 0, tiled=True)

    first = (lax.axis_index(seq) * slots).astype(jnp.int32).reshape(1)
    most = (slots + seqs * (GROUP - 1)) // GROUP
    most = (most + BATCH - 1) // BATCH * BATCH
    places = (most * GROUP) // slots * slots + slots
    smem = pl.BlockSpec(memory_space=pltpu.SMEM)
    in_hbm = pl.BlockSpec(memory_space=pltpu.HBM)
    order = pl.pallas_call(
        functools.partial(order_slots, page_len),
        out_shape=jax.ShapeDtypeStruct((1, places), jnp.int32),
        in_specs=[smem, smem, in_hbm],
        scratch_shapes=[
            pltpu.VMEM((seqs, pages), jnp.int32),
            pltpu.VMEM((slots, LANES), f32),
            pltpu.VMEM((slots, LANES), f32),
            pltpu.SemaphoreType.DMA,
        ],
        compiler_params=room(4),
    )(first, lengths, hbm(page_table))
    rope_tiles = rope_cache.reshape(slots // 8, 8, page_len * rope // LANES, LANES)
    rope_tiles = jnp.swapaxes(rope_tiles, 1, 2)
    tokens = GROUP * page_len
    rope_score = pl.pallas_call(
        functools.partial(score_rope, scale, page_len),
        out_shape=pltpu.HBM((most, heads, tokens), f32),
        in_specs=[smem, in_hbm, in_hbm],
        scratch_shapes=[
            pltpu.VMEM(q_rope.shape, bf16),
            pltpu.VMEM(rope_tiles.shape, bf16),
            pltpu.VMEM((page_len * rope * 8 // LANES, LANES), f32),
            pltpu.VMEM((8, page_len, LANES), f32),
            pltpu.VMEM((slots, page_len, LANES), bf16),
            pltpu.SemaphoreType.DMA((2,)),
        ],
        compiler_params=room(16),
    )(order, hbm(q_rope), hbm(rope_tiles))

    out_width = width + LANES
    partial, up = pl.pallas_call(
        functools.partial(attend, scale, page_len, sender_of(seq, peers_order)),
        out_shape=(
            jax.ShapeDtypeStruct((heads, seqs, out_width), bf16),
            jax.ShapeDtypeStruct((shards, cols, LANES), bf16),
        ),
        in_specs=[
            smem,
            whole(recv.shape),
            in_hbm,
            in_hbm,
        ],
        scratch_shapes=[
            pltpu.VMEM((most, tokens, width), bf16),
            pltpu.VMEM((seqs * heads, width), bf16),
            pltpu.VMEM((most, heads, tokens), f32),
            pltpu.VMEM((seqs, heads, LANES), f32),
            pltpu.VMEM((seqs, heads, LANES), f32),
            pltpu.VMEM((seqs, heads, width), f32),
            pltpu.VMEM((2, seqs * heads, LANES), f32),
            pltpu.SemaphoreType.DMA((most // BATCH,)),
            pltpu.SemaphoreType.DMA((most // BATCH,)),
        ],
        compiler_params=room(24),
    )(order, recv, hbm(rope_score), hbm(latent_cache))
    peers = lax.all_to_all(partial, peers_order, 0, 0, tiled=True)

    values = pl.pallas_call(
        functools.partial(combine, width),
        out_shape=jax.ShapeDtypeStruct((shards, seqs, value_dim), bf16),
        compiler_params=room(8),
    )(peers, up)
    every = lax.all_to_all(values, peers_order, 0, 0, tiled=True)
    flat = jnp.swapaxes(every, 0, 1).reshape(seqs, heads * value_dim)
    half = jnp.dot(flat, w_out, preferred_element_type=f32)
    both = half + lax.ppermute(half, "mp", [(0, 1), (1, 0)])
    share = half.shape[1] // lax.axis_size("mp")
    return lax.dynamic_slice_in_dim(both, lax.axis_index("mp") * share, share, 1).astype(bf16)


def sender_of(seq, peers_order):
    bits = len(seq)
    places = []
    for shard in range(2**bits):
        bit = {axis: shard >> (bits - 1 - i) & 1 for i, axis in enumerate(seq)}
        places.append(sum(bit[axis] << (bits - 1 - i) for i, axis in enumerate(peers_order)))
    return tuple(places)


def solution(mesh):
    bits = mesh.shape["seq"].bit_length() - 1
    assert mesh.shape["seq"] == 2**bits and bits % 2 == 0
    seq = tuple(f"seq_{i}" for i in range(bits))
    peers_order = seq[: bits // 2][::-1] + seq[bits // 2 :][::-1]
    finer = Mesh(
        mesh.devices.reshape(mesh.shape["groups"], *(2,) * bits, mesh.shape["mp"]),
        ("groups", *seq, "mp"),
    )
    return jax.shard_map(
        functools.partial(local, seq, peers_order),
        mesh=finer,
        in_specs=(
            P(("groups", *seq), None, None),
            P(("groups", *seq), None),
            P("groups", "mp", None),
            P("groups", "mp", None),
            P("mp", None, seq),
            P("mp", seq, None),
            P("mp", seq),
            P("groups", None),
            P("groups"),
        ),
        out_specs=P("groups", (*seq, "mp")),
        check_vma=False,
    )
```

```python
import functools

import jax
import jax.numpy as jnp
from jax import lax
from jax.experimental import pallas as pl
from jax.experimental.pallas import tpu as pltpu
from jax.sharding import Mesh
from jax.sharding import PartitionSpec as P

NEG = -1e30
LANES = 128
GROUP = 4
BATCH = 6
NT = (((1,), (1,)), ((), ()))


def whole(shape):
    return pl.BlockSpec(shape, lambda *_: (0,) * len(shape))


def room(mib):
    return pltpu.CompilerParams(vmem_limit_bytes=mib * 1024 * 1024)


def hbm(x):
    return pltpu.with_memory_space_constraint(x, pltpu.HBM)


def send_query(q_hbm, w_hbm, v_hbm, out_ref, q_ref, w_ref, v_ref, sems):
    seqs, heads, nope = q_ref.shape
    cols = w_ref.shape[1]
    moves = [
        pltpu.make_async_copy(source, target, sems.at[i])
        for i, (source, target) in enumerate(((q_hbm, q_ref), (w_hbm, w_ref), (v_hbm, v_ref)))
    ]
    for move in moves:
        move.start()
    for move in moves:
        move.wait()
    q = q_ref[...].reshape(seqs * heads, nope)
    w = w_ref[...].reshape(heads * cols, nope)
    every = lax.dot_general(w, q, NT, preferred_element_type=jnp.float32)
    every = every.reshape(heads, cols, seqs * heads)
    head = lax.broadcasted_iota(jnp.int32, every.shape, 0)
    lane = lax.broadcasted_iota(jnp.int32, every.shape, 2)
    part = jnp.sum(jnp.where(lane % heads == head, every, 0.0), axis=0).astype(jnp.bfloat16)
    shards = out_ref.shape[0]
    tiles = seqs * heads // LANES
    for tile in range(tiles):
        piece = part[:, tile * LANES : (tile + 1) * LANES]
        out_ref[:, tile * cols : (tile + 1) * cols, :] = jnp.broadcast_to(piece[None], (shards, cols, LANES))
    out_ref[:, tiles * cols :, :] = v_ref[...]


def order_slots(page_len, first_ref, lengths_ref, table_hbm, out_ref, table_ref, owner_sum, fill_sum, sem):
    seqs, pages = table_ref.shape
    slots = owner_sum.shape[0]
    places = out_ref.shape[1]
    f32, bf16 = jnp.float32, jnp.bfloat16
    logical = lax.broadcasted_iota(jnp.int32, (seqs, pages), 1)
    seq = lax.broadcasted_iota(jnp.int32, (seqs, pages), 0)
    move = pltpu.make_async_copy(table_hbm, table_ref, sem)
    move.start()
    length = jnp.zeros((seqs, pages), jnp.int32)
    for b in range(seqs):
        length = jnp.where(seq == b, lengths_ref[b], length)
    left = length - page_len * logical
    move.wait()
    local_slot = jnp.where(left > 0, table_ref[...] - first_ref[0], -1)
    tokens = jnp.clip(left, 0, page_len)
    code = (seq * LANES + tokens).astype(f32)

    def at_slot(slot, carry):
        hit = jnp.where(local_slot == slot, code, 0.0)
        acc = hit[:, :LANES]
        for j in range(1, pages // LANES):
            acc = acc + hit[:, j * LANES : (j + 1) * LANES]
        row = jnp.sum(acc, axis=0, keepdims=True)
        owner = jnp.floor(row * (1.0 / LANES))
        owner_sum[pl.ds(slot, 1), :] = owner
        fill_sum[pl.ds(slot, 1), :] = row - owner * LANES
        return carry

    lax.fori_loop(0, slots, at_slot, 0, unroll=4)
    ones = jnp.ones((8, LANES), bf16)
    owner = lax.dot_general(ones, owner_sum[...].astype(bf16), NT, preferred_element_type=f32)
    fill = lax.dot_general(ones, fill_sum[...].astype(bf16), NT, preferred_element_type=f32)

    row = lax.broadcasted_iota(jnp.int32, (seqs, slots), 0)
    slot = lax.broadcasted_iota(jnp.int32, (seqs, slots), 1)
    mine = (owner[:seqs] == row.astype(f32)) & (fill[:seqs] > 0.0)
    ours = jnp.where(mine, 1.0, 0.0)
    before = lax.broadcasted_iota(jnp.int32, (slots, slots), 0) < lax.broadcasted_iota(
        jnp.int32, (slots, slots), 1
    )
    rank = jnp.dot(ours.astype(bf16), jnp.where(before, 1.0, 0.0).astype(bf16), preferred_element_type=f32)
    count = jnp.broadcast_to(jnp.sum(ours, axis=1, keepdims=True), (seqs, slots))
    groups = jnp.floor((count + (GROUP - 1)) * (1.0 / GROUP))
    base, starts = jnp.zeros((1, slots), f32), []
    for b in range(seqs):
        starts.append(base)
        base = base + groups[b : b + 1]
    place = GROUP * jnp.concatenate(starts, axis=0) + rank
    place = jnp.sum(jnp.where(mine, place + 1.0, 0.0), axis=0, keepdims=True) - 1.0
    at = lax.broadcasted_iota(jnp.int32, (places, slots), 0).astype(f32) == place
    value = jnp.where(row == 0, slot.astype(f32), jnp.where(row == 1, fill[:seqs], owner[:seqs]))
    found = lax.dot_general(
        value.astype(bf16), jnp.where(at, 1.0, 0.0).astype(bf16), NT, preferred_element_type=f32
    )
    packed = (found[2:3] * LANES + found[0:1]) * LANES + found[1:2]
    place = lax.broadcasted_iota(jnp.int32, (1, places), 1)
    total = jnp.concatenate([base] * (places // slots), axis=1)
    out_ref[...] = jnp.where(place == places - 1, total, packed).astype(jnp.int32)


SHIFT = 7


def steps_of(order_ref, batch):
    return (order_ref[0, order_ref.shape[1] - 1] + (batch - 1)) // batch


def slot_at(order_ref, group, k):
    code = order_ref[0, GROUP * group + k]
    return lax.shift_right_logical(code, SHIFT) & (LANES - 1), code & (LANES - 1)


def owner_of(order_ref, group):
    return lax.shift_right_logical(order_ref[0, GROUP * group], 2 * SHIFT)


def score_rope(
    scale, page_len, order_ref, q_hbm, tiles_hbm, out_ref, q_ref, tiles, flat, spread, keys, sems
):
    heads, rope = q_ref.shape[1:]
    blocks, pairs, _, _ = tiles.shape
    first = pltpu.make_async_copy(q_hbm, q_ref, sems.at[0])
    second = pltpu.make_async_copy(tiles_hbm, tiles, sems.at[1])
    first.start()
    second.start()
    first.wait()
    second.wait()
    even = lax.broadcasted_iota(jnp.int32, (pairs, LANES), 1) < rope

    def spread_block(block, carry):
        flat[...] = tiles[block].astype(jnp.float32).reshape(pairs * 8, LANES)
        for k in range(8):
            two = flat[pl.ds(k, pairs, stride=8), :]
            spread[k, pl.ds(0, pairs, stride=2), :] = jnp.where(even, two, 0.0)
            spread[k, pl.ds(1, pairs, stride=2), :] = jnp.where(even, 0.0, two)
        keys[pl.ds(block * 8, 8)] = spread[...].astype(jnp.bfloat16)
        return carry

    lax.fori_loop(0, blocks, spread_block, 0)
    lane = lax.broadcasted_iota(jnp.int32, (heads, GROUP * page_len), 1)

    def score(step, carry):
        for j in range(BATCH):
            group = step * BATCH + j
            rows, limit = [], None
            for k in range(GROUP):
                slot, fill = slot_at(order_ref, group, k)
                rows.append(keys[slot])
                end = k * page_len + fill
                limit = end if limit is None else jnp.where(lane >= k * page_len, end, limit)
            query = q_ref[owner_of(order_ref, group)].astype(jnp.float32)
            query = jnp.concatenate([query, query], axis=1).astype(jnp.bfloat16)
            both = lax.dot_general(
                query, jnp.concatenate(rows, axis=0), NT, preferred_element_type=jnp.float32
            )
            out_ref[group] = jnp.where(lane < limit, both * scale, NEG)
        return carry

    lax.fori_loop(0, steps_of(order_ref, BATCH), score, 0)


def attend(
    scale, page_len, sender, order_ref, recv_ref, rope_hbm, latent_hbm, out_ref, up_ref,
    latent, query, scores, top, total, acc, rows, sems, rope_sems,
):
    _, tokens, width = latent.shape
    seqs, heads, _ = top.shape
    steps = steps_of(order_ref, BATCH)

    def fetch(step):
        for j in range(BATCH):
            group = step * BATCH + j
            for k in range(GROUP):
                slot, _ = slot_at(order_ref, group, k)
                pltpu.make_async_copy(
                    latent_hbm.at[slot], latent.at[group, pl.ds(k * page_len, page_len)], sems.at[step]
                ).start()
        batch = pl.ds(step * BATCH, BATCH)
        pltpu.make_async_copy(rope_hbm.at[batch], scores.at[batch], rope_sems.at[step]).start()

    ahead = 2
    for step in range(ahead):

        @pl.when(step < steps)
        def _():
            fetch(step)

    cols = recv_ref.shape[1] // (seqs * heads // LANES + 1)
    for tile in range(seqs * heads // LANES):
        block = recv_ref[:, tile * cols : (tile + 1) * cols, :].astype(jnp.float32)
        block = jnp.concatenate([block[at] for at in sender], axis=0)
        query[tile * LANES : (tile + 1) * LANES, :] = block.T.astype(jnp.bfloat16)
    for shard, at in enumerate(sender):
        up_ref[shard] = recv_ref[at, recv_ref.shape[1] - cols :, :]
    top[...] = jnp.full(top.shape, NEG, jnp.float32)
    total[...] = jnp.zeros(total.shape, jnp.float32)
    acc[...] = jnp.zeros(acc.shape, jnp.float32)

    def score(step, carry):
        @pl.when(step + ahead < steps)
        def _():
            fetch(step + ahead)

        batch = pl.ds(step * BATCH, BATCH)
        pltpu.make_async_copy(latent.at[batch], latent.at[batch], sems.at[step]).wait()
        pltpu.make_async_copy(rope_hbm.at[batch], scores.at[batch], rope_sems.at[step]).wait()
        made = []
        for j in range(BATCH):
            group = step * BATCH + j
            b = owner_of(order_ref, group)
            lhs = query[pl.ds(pl.multiple_of(b * heads, heads), heads), :]
            both = lax.dot_general(lhs, latent[group], NT, preferred_element_type=jnp.float32)
            made.append((group, b, both * scale + scores[group]))
        for group, b, both in made:
            scores[group] = both
            high = both[:, :LANES]
            for k in range(1, tokens // LANES):
                high = jnp.maximum(high, both[:, k * LANES : (k + 1) * LANES])
            top[b] = jnp.maximum(top[b], high)
        return carry

    lax.fori_loop(0, steps, score, 0)

    for b in range(seqs):
        top[b] = jnp.broadcast_to(jnp.max(top[b], axis=1, keepdims=True), (heads, LANES))

    def weigh(step, carry):
        made = []
        for j in range(BATCH):
            group = step * BATCH + j
            b = owner_of(order_ref, group)
            both = scores[group]
            peak = top[b]
            parts, some = [], None
            for k in range(tokens // LANES):
                part = both[:, k * LANES : (k + 1) * LANES]
                part = jnp.where(part > 0.5 * NEG, jnp.exp(part - peak), 0.0)
                some = part if some is None else some + part
                parts.append(part.astype(jnp.bfloat16))
            lhs = jnp.concatenate(parts, axis=1)
            made.append((b, some, jnp.dot(lhs, latent[group], preferred_element_type=jnp.float32)))
        for b, some, out in made:
            total[b] = total[b] + some
            acc[b] = acc[b] + out
        return carry

    lax.fori_loop(0, steps, weigh, 0)

    lane = lax.broadcasted_iota(jnp.int32, (heads, LANES), 1)
    for piece in range(width // LANES + 1):
        for b in range(seqs):
            if piece < width // LANES:
                value = acc[b, :, piece * LANES : (piece + 1) * LANES]
            else:
                sums = jnp.broadcast_to(jnp.sum(total[b], axis=1, keepdims=True), (heads, LANES))
                value = jnp.where(lane < 3, top[b], sums)
            rows[piece % 2, pl.ds(b, heads, stride=seqs), :] = value
        value = rows[piece % 2]
        if piece == width // LANES:
            high = value.astype(jnp.bfloat16).astype(jnp.float32)
            middle = (value - high).astype(jnp.bfloat16).astype(jnp.float32)
            low = value - high - middle
            third = lax.broadcasted_iota(jnp.int32, value.shape, 1) % 3
            value = jnp.where(third == 0, high, jnp.where(third == 1, middle, low))
        out_ref[:, :, piece * LANES : (piece + 1) * LANES] = value.reshape(heads, seqs, LANES).astype(jnp.bfloat16)


def combine(width, peers_ref, up_ref, out_ref):
    shards, seqs, _ = peers_ref.shape
    stats = peers_ref[:, :, width:].astype(jnp.float32)
    lane = lax.broadcasted_iota(jnp.int32, stats.shape, 2)
    peak = jnp.sum(jnp.where(lane < 3, stats, 0.0), axis=2, keepdims=True)
    sums = jnp.sum(jnp.where((lane >= 3) & (lane < 6), stats, 0.0), axis=2, keepdims=True)
    rescale = jnp.exp(peak - jnp.max(peak, axis=0, keepdims=True))
    total = jnp.sum(sums * rescale, axis=0)
    mixed = jnp.sum(peers_ref[:, :, :width].astype(jnp.float32) * rescale, axis=0)
    attention = (mixed / total).astype(jnp.bfloat16)
    up = up_ref[...].astype(jnp.float32).reshape(width, up_ref.shape[2]).astype(jnp.bfloat16)
    values = jnp.dot(attention, up, preferred_element_type=jnp.float32).astype(jnp.bfloat16)
    out_ref[...] = jnp.broadcast_to(values[None], out_ref.shape)


def local(
    seq, peers_order,
    latent_cache, rope_cache, q_nope, q_rope, w_uk, value_up_weight, w_out, page_table, lengths,
):
    slots, page_len, width = latent_cache.shape
    seqs, heads, nope = q_nope.shape
    rope = q_rope.shape[2]
    value_dim = value_up_weight.shape[2]
    cols = w_uk.shape[2]
    shards = lax.axis_size(seq)
    pages = page_table.shape[1]
    scale = (nope + rope) ** -0.5
    f32, bf16 = jnp.float32, jnp.bfloat16

    send_rows = (seqs * heads // LANES + 1) * cols
    sent = pl.pallas_call(
        send_query,
        in_specs=[pl.BlockSpec(memory_space=pltpu.HBM)] * 3,
        out_shape=jax.ShapeDtypeStruct((shards, send_rows, LANES), bf16),
        scratch_shapes=[
            pltpu.VMEM(q_nope.shape, bf16),
            pltpu.VMEM((heads, cols, nope), bf16),
            pltpu.VMEM(value_up_weight.shape, bf16),
            pltpu.SemaphoreType.DMA((3,)),
        ],
        compiler_params=room(8),
    )(hbm(q_nope), hbm(jnp.swapaxes(w_uk, 1, 2)), hbm(value_up_weight))
    recv = lax.all_to_all(sent, peers_order, 0, 0, tiled=True)

    first = (lax.axis_index(seq) * slots).astype(jnp.int32).reshape(1)
    most = (slots + seqs * (GROUP - 1)) // GROUP
    most = (most + BATCH - 1) // BATCH * BATCH
    places = (most * GROUP) // slots * slots + slots
    smem = pl.BlockSpec(memory_space=pltpu.SMEM)
    in_hbm = pl.BlockSpec(memory_space=pltpu.HBM)
    order = pl.pallas_call(
        functools.partial(order_slots, page_len),
        out_shape=jax.ShapeDtypeStruct((1, places), jnp.int32),
        in_specs=[smem, smem, in_hbm],
        scratch_shapes=[
            pltpu.VMEM((seqs, pages), jnp.int32),
            pltpu.VMEM((slots, LANES), f32),
            pltpu.VMEM((slots, LANES), f32),
            pltpu.SemaphoreType.DMA,
        ],
        compiler_params=room(4),
    )(first, lengths, hbm(page_table))
    rope_tiles = rope_cache.reshape(slots // 8, 8, page_len * rope // LANES, LANES)
    rope_tiles = jnp.swapaxes(rope_tiles, 1, 2)
    tokens = GROUP * page_len
    rope_score = pl.pallas_call(
        functools.partial(score_rope, scale, page_len),
        out_shape=pltpu.HBM((most, heads, tokens), f32),
        in_specs=[smem, in_hbm, in_hbm],
        scratch_shapes=[
            pltpu.VMEM(q_rope.shape, bf16),
            pltpu.VMEM(rope_tiles.shape, bf16),
            pltpu.VMEM((page_len * rope * 8 // LANES, LANES), f32),
            pltpu.VMEM((8, page_len, LANES), f32),
            pltpu.VMEM((slots, page_len, LANES), bf16),
            pltpu.SemaphoreType.DMA((2,)),
        ],
        compiler_params=room(16),
    )(order, hbm(q_rope), hbm(rope_tiles))

    out_width = width + LANES
    partial, up = pl.pallas_call(
        functools.partial(attend, scale, page_len, sender_of(seq, peers_order)),
        out_shape=(
            jax.ShapeDtypeStruct((heads, seqs, out_width), bf16),
            jax.ShapeDtypeStruct((shards, cols, LANES), bf16),
        ),
        in_specs=[
            smem,
            whole(recv.shape),
            in_hbm,
            in_hbm,
        ],
        scratch_shapes=[
            pltpu.VMEM((most, tokens, width), bf16),
            pltpu.VMEM((seqs * heads, width), bf16),
            pltpu.VMEM((most, heads, tokens), f32),
            pltpu.VMEM((seqs, heads, LANES), f32),
            pltpu.VMEM((seqs, heads, LANES), f32),
            pltpu.VMEM((seqs, heads, width), f32),
            pltpu.VMEM((2, seqs * heads, LANES), f32),
            pltpu.SemaphoreType.DMA((most // BATCH,)),
            pltpu.SemaphoreType.DMA((most // BATCH,)),
        ],
        compiler_params=room(24),
    )(order, recv, hbm(rope_score), hbm(latent_cache))
    peers = lax.all_to_all(partial, peers_order, 0, 0, tiled=True)

    values = pl.pallas_call(
        functools.partial(combine, width),
        out_shape=jax.ShapeDtypeStruct((shards, seqs, value_dim), bf16),
        compiler_params=room(8),
    )(peers, up)
    every = lax.all_to_all(values, peers_order, 0, 0, tiled=True)
    flat = jnp.swapaxes(every, 0, 1).reshape(seqs, heads * value_dim)
    half = jnp.dot(flat, w_out, preferred_element_type=f32)
    both = half + lax.ppermute(half, "mp", [(0, 1), (1, 0)])
    share = half.shape[1] // lax.axis_size("mp")
    return lax.dynamic_slice_in_dim(both, lax.axis_index("mp") * share, share, 1).astype(bf16)


def sender_of(seq, peers_order):
    bits = len(seq)
    places = []
    for shard in range(2**bits):
        bit = {axis: shard >> (bits - 1 - i) & 1 for i, axis in enumerate(seq)}
        places.append(sum(bit[axis] << (bits - 1 - i) for i, axis in enumerate(peers_order)))
    return tuple(places)


def solution(mesh):
    bits = mesh.shape["seq"].bit_length() - 1
    assert mesh.shape["seq"] == 2**bits and bits % 2 == 0
    seq = tuple(f"seq_{i}" for i in range(bits))
    peers_order = seq[: bits // 2][::-1] + seq[bits // 2 :][::-1]
    finer = Mesh(
        mesh.devices.reshape(mesh.shape["groups"], *(2,) * bits, mesh.shape["mp"]),
        ("groups", *seq, "mp"),
    )
    return jax.shard_map(
        functools.partial(local, seq, peers_order),
        mesh=finer,
        in_specs=(
            P(("groups", *seq), None, None),
            P(("groups", *seq), None),
            P("groups", "mp", None),
            P("groups", "mp", None),
            P("mp", None, seq),
            P("mp", seq, None),
            P("mp", seq),
            P("groups", None),
            P("groups"),
        ),
        out_specs=P("groups", (*seq, "mp")),
        check_vma=False,
    )
```

```python
import functools

import jax
import jax.numpy as jnp
from jax import lax
from jax.experimental import pallas as pl
from jax.experimental.pallas import tpu as pltpu
from jax.sharding import Mesh
from jax.sharding import PartitionSpec as P

NEG = -1e30
LANES = 128
GROUP = 4
BATCH = 6
NT = (((1,), (1,)), ((), ()))


def whole(shape):
    return pl.BlockSpec(shape, lambda *_: (0,) * len(shape))


def room(mib):
    return pltpu.CompilerParams(vmem_limit_bytes=mib * 1024 * 1024)


def hbm(x):
    return pltpu.with_memory_space_constraint(x, pltpu.HBM)


def send_query(q_hbm, w_hbm, v_hbm, out_ref, q_ref, w_ref, v_ref, sems):
    seqs, heads, nope = q_ref.shape
    cols = w_ref.shape[1]
    moves = [
        pltpu.make_async_copy(source, target, sems.at[i])
        for i, (source, target) in enumerate(((q_hbm, q_ref), (w_hbm, w_ref), (v_hbm, v_ref)))
    ]
    for move in moves:
        move.start()
    for move in moves:
        move.wait()
    q = q_ref[...].reshape(seqs * heads, nope)
    w = w_ref[...].reshape(heads * cols, nope)
    every = lax.dot_general(w, q, NT, preferred_element_type=jnp.float32)
    every = every.reshape(heads, cols, seqs * heads)
    head = lax.broadcasted_iota(jnp.int32, every.shape, 0)
    lane = lax.broadcasted_iota(jnp.int32, every.shape, 2)
    part = jnp.sum(jnp.where(lane % heads == head, every, 0.0), axis=0).astype(jnp.bfloat16)
    shards = out_ref.shape[0]
    tiles = seqs * heads // LANES
    for tile in range(tiles):
        piece = part[:, tile * LANES : (tile + 1) * LANES]
        out_ref[:, tile * cols : (tile + 1) * cols, :] = jnp.broadcast_to(piece[None], (shards, cols, LANES))
    out_ref[:, tiles * cols :, :] = v_ref[...]


def order_slots(page_len, first_ref, lengths_ref, table_hbm, out_ref, table_ref, owner_sum, fill_sum, sem):
    seqs, pages = table_ref.shape
    slots = owner_sum.shape[0]
    places = out_ref.shape[1]
    f32, bf16 = jnp.float32, jnp.bfloat16
    logical = lax.broadcasted_iota(jnp.int32, (seqs, pages), 1)
    seq = lax.broadcasted_iota(jnp.int32, (seqs, pages), 0)
    move = pltpu.make_async_copy(table_hbm, table_ref, sem)
    move.start()
    length = jnp.zeros((seqs, pages), jnp.int32)
    for b in range(seqs):
        length = jnp.where(seq == b, lengths_ref[b], length)
    left = length - page_len * logical
    move.wait()
    local_slot = jnp.where(left > 0, table_ref[...] - first_ref[0], -1)
    tokens = jnp.clip(left, 0, page_len)
    code = (seq * LANES + tokens).astype(f32)

    def at_slot(slot, carry):
        hit = jnp.where(local_slot == slot, code, 0.0)
        acc = hit[:, :LANES]
        for j in range(1, pages // LANES):
            acc = acc + hit[:, j * LANES : (j + 1) * LANES]
        row = jnp.sum(acc, axis=0, keepdims=True)
        owner = jnp.floor(row * (1.0 / LANES))
        owner_sum[pl.ds(slot, 1), :] = owner
        fill_sum[pl.ds(slot, 1), :] = row - owner * LANES
        return carry

    lax.fori_loop(0, slots, at_slot, 0, unroll=4)
    ones = jnp.ones((8, LANES), bf16)
    owner = lax.dot_general(ones, owner_sum[...].astype(bf16), NT, preferred_element_type=f32)
    fill = lax.dot_general(ones, fill_sum[...].astype(bf16), NT, preferred_element_type=f32)

    row = lax.broadcasted_iota(jnp.int32, (seqs, slots), 0)
    slot = lax.broadcasted_iota(jnp.int32, (seqs, slots), 1)
    mine = (owner[:seqs] == row.astype(f32)) & (fill[:seqs] > 0.0)
    ours = jnp.where(mine, 1.0, 0.0)
    before = lax.broadcasted_iota(jnp.int32, (slots, slots), 0) < lax.broadcasted_iota(
        jnp.int32, (slots, slots), 1
    )
    rank = jnp.dot(ours.astype(bf16), jnp.where(before, 1.0, 0.0).astype(bf16), preferred_element_type=f32)
    count = jnp.broadcast_to(jnp.sum(ours, axis=1, keepdims=True), (seqs, slots))
    groups = jnp.floor((count + (GROUP - 1)) * (1.0 / GROUP))
    base, starts = jnp.zeros((1, slots), f32), []
    for b in range(seqs):
        starts.append(base)
        base = base + groups[b : b + 1]
    place = GROUP * jnp.concatenate(starts, axis=0) + rank
    place = jnp.sum(jnp.where(mine, place + 1.0, 0.0), axis=0, keepdims=True) - 1.0
    at = lax.broadcasted_iota(jnp.int32, (places, slots), 0).astype(f32) == place
    value = jnp.where(row == 0, slot.astype(f32), jnp.where(row == 1, fill[:seqs], owner[:seqs]))
    found = lax.dot_general(
        value.astype(bf16), jnp.where(at, 1.0, 0.0).astype(bf16), NT, preferred_element_type=f32
    )
    packed = (found[2:3] * LANES + found[0:1]) * LANES + found[1:2]
    place = lax.broadcasted_iota(jnp.int32, (1, places), 1)
    total = jnp.concatenate([base] * (places // slots), axis=1)
    out_ref[...] = jnp.where(place == places - 1, total, packed).astype(jnp.int32)


SHIFT = 7


def steps_of(order_ref, batch):
    return (order_ref[0, order_ref.shape[1] - 1] + (batch - 1)) // batch


def slot_at(order_ref, group, k):
    code = order_ref[0, GROUP * group + k]
    return lax.shift_right_logical(code, SHIFT) & (LANES - 1), code & (LANES - 1)


def owner_of(order_ref, group):
    return lax.shift_right_logical(order_ref[0, GROUP * group], 2 * SHIFT)


def score_rope(
    scale, page_len, order_ref, q_hbm, tiles_hbm, out_ref, q_ref, tiles, flat, spread, keys, sems
):
    heads, rope = q_ref.shape[1:]
    blocks, pairs, _, _ = tiles.shape
    first = pltpu.make_async_copy(q_hbm, q_ref, sems.at[0])
    second = pltpu.make_async_copy(tiles_hbm, tiles, sems.at[1])
    first.start()
    second.start()
    first.wait()
    second.wait()
    even = lax.broadcasted_iota(jnp.int32, (pairs, LANES), 1) < rope

    def spread_block(block, carry):
        flat[...] = tiles[block].astype(jnp.float32).reshape(pairs * 8, LANES)
        for k in range(8):
            two = flat[pl.ds(k, pairs, stride=8), :]
            spread[k, pl.ds(0, pairs, stride=2), :] = jnp.where(even, two, 0.0)
            spread[k, pl.ds(1, pairs, stride=2), :] = jnp.where(even, 0.0, two)
        keys[pl.ds(block * 8, 8)] = spread[...].astype(jnp.bfloat16)
        return carry

    lax.fori_loop(0, blocks, spread_block, 0)
    lane = lax.broadcasted_iota(jnp.int32, (heads, GROUP * page_len), 1)

    def score(step, carry):
        for j in range(BATCH):
            group = step * BATCH + j
            rows, limit = [], None
            for k in range(GROUP):
                slot, fill = slot_at(order_ref, group, k)
                rows.append(keys[slot])
                end = k * page_len + fill
                limit = end if limit is None else jnp.where(lane >= k * page_len, end, limit)
            query = q_ref[owner_of(order_ref, group)].astype(jnp.float32)
            query = jnp.concatenate([query, query], axis=1).astype(jnp.bfloat16)
            both = lax.dot_general(
                query, jnp.concatenate(rows, axis=0), NT, preferred_element_type=jnp.float32
            )
            out_ref[group] = jnp.where(lane < limit, both * scale, NEG)
        return carry

    lax.fori_loop(0, steps_of(order_ref, BATCH), score, 0)


def attend(
    scale, page_len, sender, order_ref, recv_ref, rope_hbm, latent_hbm, out_ref, up_ref,
    latent, query, scores, top, total, acc, rows, sems, rope_sems,
):
    _, tokens, width = latent.shape
    seqs, heads, _ = top.shape
    steps = steps_of(order_ref, BATCH)

    def fetch(step):
        for j in range(BATCH):
            group = step * BATCH + j
            for k in range(GROUP):
                slot, _ = slot_at(order_ref, group, k)
                pltpu.make_async_copy(
                    latent_hbm.at[slot], latent.at[group, pl.ds(k * page_len, page_len)], sems.at[step]
                ).start()
        batch = pl.ds(step * BATCH, BATCH)
        pltpu.make_async_copy(rope_hbm.at[batch], scores.at[batch], rope_sems.at[step]).start()

    ahead = 2
    for step in range(ahead):

        @pl.when(step < steps)
        def _():
            fetch(step)

    cols = recv_ref.shape[1] // (seqs * heads // LANES + 1)
    for tile in range(seqs * heads // LANES):
        block = recv_ref[:, tile * cols : (tile + 1) * cols, :].astype(jnp.float32)
        block = jnp.concatenate([block[at] for at in sender], axis=0)
        query[tile * LANES : (tile + 1) * LANES, :] = block.T.astype(jnp.bfloat16)
    for shard, at in enumerate(sender):
        up_ref[shard] = recv_ref[at, recv_ref.shape[1] - cols :, :]
    top[...] = jnp.full(top.shape, NEG, jnp.float32)
    total[...] = jnp.zeros(total.shape, jnp.float32)
    acc[...] = jnp.zeros(acc.shape, jnp.float32)

    def score(step, carry):
        @pl.when(step + ahead < steps)
        def _():
            fetch(step + ahead)

        batch = pl.ds(step * BATCH, BATCH)
        pltpu.make_async_copy(latent.at[batch], latent.at[batch], sems.at[step]).wait()
        pltpu.make_async_copy(rope_hbm.at[batch], scores.at[batch], rope_sems.at[step]).wait()
        made = []
        for j in range(BATCH):
            group = step * BATCH + j
            b = owner_of(order_ref, group)
            lhs = query[pl.ds(pl.multiple_of(b * heads, heads), heads), :]
            both = lax.dot_general(lhs, latent[group], NT, preferred_element_type=jnp.float32)
            made.append((group, b, both * scale + scores[group]))
        for group, b, both in made:
            scores[group] = both
            high = both[:, :LANES]
            for k in range(1, tokens // LANES):
                high = jnp.maximum(high, both[:, k * LANES : (k + 1) * LANES])
            top[b] = jnp.maximum(top[b], high)
        return carry

    lax.fori_loop(0, steps, score, 0)

    for b in range(seqs):
        top[b] = jnp.broadcast_to(jnp.max(top[b], axis=1, keepdims=True), (heads, LANES))

    def weigh(step, carry):
        made = []
        for j in range(BATCH):
            group = step * BATCH + j
            b = owner_of(order_ref, group)
            both = scores[group]
            peak = top[b]
            parts, some = [], None
            for k in range(tokens // LANES):
                part = both[:, k * LANES : (k + 1) * LANES]
                part = jnp.where(part > 0.5 * NEG, jnp.exp(part - peak), 0.0)
                some = part if some is None else some + part
                parts.append(part.astype(jnp.bfloat16))
            lhs = jnp.concatenate(parts, axis=1)
            made.append((b, some, jnp.dot(lhs, latent[group], preferred_element_type=jnp.float32)))
        for b, some, out in made:
            total[b] = total[b] + some
            acc[b] = acc[b] + out
        return carry

    lax.fori_loop(0, steps, weigh, 0)

    lane = lax.broadcasted_iota(jnp.int32, (heads, LANES), 1)
    for piece in range(width // LANES + 1):
        for b in range(seqs):
            if piece < width // LANES:
                value = acc[b, :, piece * LANES : (piece + 1) * LANES]
            else:
                sums = jnp.broadcast_to(jnp.sum(total[b], axis=1, keepdims=True), (heads, LANES))
                value = jnp.where(lane < 3, top[b], sums)
            rows[piece % 2, pl.ds(b, heads, stride=seqs), :] = value
        value = rows[piece % 2]
        if piece == width // LANES:
            high = value.astype(jnp.bfloat16).astype(jnp.float32)
            middle = (value - high).astype(jnp.bfloat16).astype(jnp.float32)
            low = value - high - middle
            third = lax.broadcasted_iota(jnp.int32, value.shape, 1) % 3
            value = jnp.where(third == 0, high, jnp.where(third == 1, middle, low))
        out_ref[:, :, piece * LANES : (piece + 1) * LANES] = value.reshape(heads, seqs, LANES).astype(jnp.bfloat16)


def combine(width, peers_ref, up_ref, out_ref):
    shards, seqs, _ = peers_ref.shape
    stats = peers_ref[:, :, width:].astype(jnp.float32)
    lane = lax.broadcasted_iota(jnp.int32, stats.shape, 2)
    peak = jnp.sum(jnp.where(lane < 3, stats, 0.0), axis=2, keepdims=True)
    sums = jnp.sum(jnp.where((lane >= 3) & (lane < 6), stats, 0.0), axis=2, keepdims=True)
    rescale = jnp.exp(peak - jnp.max(peak, axis=0, keepdims=True))
    total = jnp.sum(sums * rescale, axis=0)
    mixed = jnp.sum(peers_ref[:, :, :width].astype(jnp.float32) * rescale, axis=0)
    attention = (mixed / total).astype(jnp.bfloat16)
    up = up_ref[...].astype(jnp.float32).reshape(width, up_ref.shape[2]).astype(jnp.bfloat16)
    values = jnp.dot(attention, up, preferred_element_type=jnp.float32).astype(jnp.bfloat16)
    out_ref[...] = jnp.broadcast_to(values[None], out_ref.shape)


def local(
    seq, peers_order,
    latent_cache, rope_cache, q_nope, q_rope, w_uk, value_up_weight, w_out, page_table, lengths,
):
    slots, page_len, width = latent_cache.shape
    seqs, heads, nope = q_nope.shape
    rope = q_rope.shape[2]
    value_dim = value_up_weight.shape[2]
    cols = w_uk.shape[2]
    shards = lax.axis_size(seq)
    pages = page_table.shape[1]
    scale = (nope + rope) ** -0.5
    f32, bf16 = jnp.float32, jnp.bfloat16

    send_rows = (seqs * heads // LANES + 1) * cols
    sent = pl.pallas_call(
        send_query,
        in_specs=[pl.BlockSpec(memory_space=pltpu.HBM)] * 3,
        out_shape=jax.ShapeDtypeStruct((shards, send_rows, LANES), bf16),
        scratch_shapes=[
            pltpu.VMEM(q_nope.shape, bf16),
            pltpu.VMEM((heads, cols, nope), bf16),
            pltpu.VMEM(value_up_weight.shape, bf16),
            pltpu.SemaphoreType.DMA((3,)),
        ],
        compiler_params=room(8),
    )(hbm(q_nope), hbm(jnp.swapaxes(w_uk, 1, 2)), hbm(value_up_weight))
    recv = lax.all_to_all(sent, peers_order, 0, 0, tiled=True)

    first = (lax.axis_index(seq) * slots).astype(jnp.int32).reshape(1)
    most = (slots + seqs * (GROUP - 1)) // GROUP
    most = (most + BATCH - 1) // BATCH * BATCH
    places = (most * GROUP) // slots * slots + slots
    smem = pl.BlockSpec(memory_space=pltpu.SMEM)
    in_hbm = pl.BlockSpec(memory_space=pltpu.HBM)
    order = pl.pallas_call(
        functools.partial(order_slots, page_len),
        out_shape=jax.ShapeDtypeStruct((1, places), jnp.int32),
        in_specs=[smem, smem, in_hbm],
        scratch_shapes=[
            pltpu.VMEM((seqs, pages), jnp.int32),
            pltpu.VMEM((slots, LANES), f32),
            pltpu.VMEM((slots, LANES), f32),
            pltpu.SemaphoreType.DMA,
        ],
        compiler_params=room(4),
    )(first, lengths, hbm(page_table))
    rope_tiles = rope_cache.reshape(slots // 8, 8, page_len * rope // LANES, LANES)
    rope_tiles = jnp.swapaxes(rope_tiles, 1, 2)
    tokens = GROUP * page_len
    rope_score = pl.pallas_call(
        functools.partial(score_rope, scale, page_len),
        out_shape=pltpu.HBM((most, heads, tokens), f32),
        in_specs=[smem, in_hbm, in_hbm],
        scratch_shapes=[
            pltpu.VMEM(q_rope.shape, bf16),
            pltpu.VMEM(rope_tiles.shape, bf16),
            pltpu.VMEM((page_len * rope * 8 // LANES, LANES), f32),
            pltpu.VMEM((8, page_len, LANES), f32),
            pltpu.VMEM((slots, page_len, LANES), bf16),
            pltpu.SemaphoreType.DMA((2,)),
        ],
        compiler_params=room(16),
    )(order, hbm(q_rope), hbm(rope_tiles))

    out_width = width + LANES
    partial, up = pl.pallas_call(
        functools.partial(attend, scale, page_len, sender_of(seq, peers_order)),
        out_shape=(
            jax.ShapeDtypeStruct((heads, seqs, out_width), bf16),
            jax.ShapeDtypeStruct((shards, cols, LANES), bf16),
        ),
        in_specs=[
            smem,
            whole(recv.shape),
            in_hbm,
            in_hbm,
        ],
        scratch_shapes=[
            pltpu.VMEM((most, tokens, width), bf16),
            pltpu.VMEM((seqs * heads, width), bf16),
            pltpu.VMEM((most, heads, tokens), f32),
            pltpu.VMEM((seqs, heads, LANES), f32),
            pltpu.VMEM((seqs, heads, LANES), f32),
            pltpu.VMEM((seqs, heads, width), f32),
            pltpu.VMEM((2, seqs * heads, LANES), f32),
            pltpu.SemaphoreType.DMA((most // BATCH,)),
            pltpu.SemaphoreType.DMA((most // BATCH,)),
        ],
        compiler_params=room(24),
    )(order, recv, hbm(rope_score), hbm(latent_cache))
    peers = lax.all_to_all(partial, peers_order, 0, 0, tiled=True)

    values = pl.pallas_call(
        functools.partial(combine, width),
        out_shape=jax.ShapeDtypeStruct((shards, seqs, value_dim), bf16),
        compiler_params=room(8),
    )(peers, up)
    every = lax.all_to_all(values, peers_order, 0, 0, tiled=True)
    flat = jnp.swapaxes(every, 0, 1).reshape(seqs, heads * value_dim)
    half = jnp.dot(flat, w_out, preferred_element_type=f32)
    other = lax.ppermute(half, "mp", [(0, 1), (1, 0)])
    assert lax.axis_size("mp") == 2
    share = half.shape[1] // 2
    low = lax.axis_index("mp") == 0
    mine = jnp.where(low, half[:, :share], half[:, share:])
    return (mine + jnp.where(low, other[:, :share], other[:, share:])).astype(bf16)


def sender_of(seq, peers_order):
    bits = len(seq)
    places = []
    for shard in range(2**bits):
        bit = {axis: shard >> (bits - 1 - i) & 1 for i, axis in enumerate(seq)}
        places.append(sum(bit[axis] << (bits - 1 - i) for i, axis in enumerate(peers_order)))
    return tuple(places)


def solution(mesh):
    bits = mesh.shape["seq"].bit_length() - 1
    assert mesh.shape["seq"] == 2**bits and bits % 2 == 0
    seq = tuple(f"seq_{i}" for i in range(bits))
    peers_order = seq[: bits // 2][::-1] + seq[bits // 2 :][::-1]
    finer = Mesh(
        mesh.devices.reshape(mesh.shape["groups"], *(2,) * bits, mesh.shape["mp"]),
        ("groups", *seq, "mp"),
    )
    return jax.shard_map(
        functools.partial(local, seq, peers_order),
        mesh=finer,
        in_specs=(
            P(("groups", *seq), None, None),
            P(("groups", *seq), None),
            P("groups", "mp", None),
            P("groups", "mp", None),
            P("mp", None, seq),
            P("mp", seq, None),
            P("mp", seq),
            P("groups", None),
            P("groups"),
        ),
        out_specs=P("groups", (*seq, "mp")),
        check_vma=False,
    )
```
